128 devices in a mesh: dp: 8 (over x, core), fsdp: 8 (over z_lo, y), mp: 2 (over z_hi).
Axes of the slice: x: 4, y: 4, z: 4 (z_hi: 2, z_lo: 2; z = z_hi * 2 + z_lo), core: 2. Of those that a mesh axis runs over, the one named last changes fastest.
Arguments:
- tokens_in: bfloat16 [16384, 3072], P(('dp', 'fsdp', 'mp')), may hold values from -40 to 40
- segment_ids: int32 [16384], P(('dp', 'fsdp', 'mp')), may hold values from 0 to 63, never falling along the last dimension, each value on 1 to 1024 neighbouring positions
- target_ids: int32 [16384], P(('dp', 'fsdp', 'mp')), may hold values from 0 to 16383
- old_weights: bfloat16 [4, 3072, 4096], P(None, ('dp', 'fsdp', 'mp'))
- old_first: float32 [4, 3072, 4096], P(None, ('dp', 'fsdp', 'mp')), may hold values from -6 to 6
- old_second: float32 [4, 3072, 4096], P(None, ('dp', 'fsdp', 'mp')), may hold values from 0.01 to 4
- old_block: int32 [128], P(('dp', 'fsdp', 'mp')), may hold values from 0 to 127, each once
- new_residue: int32 [8], P('dp'), may hold values from 0 to 7, each once
- norm_gain: float32 [3072], replicated, may hold values from 0.5 to 1.5
- head_weight: bfloat16 [3072, 16384], P(None, ('fsdp', 'mp'))
Outputs:
- new_weights: bfloat16 [4, 3072, 4096], P(None, 'dp', ('fsdp', 'mp'))
- new_first: float32 [4, 3072, 4096], P(None, 'dp', ('fsdp', 'mp'))
- new_second: float32 [4, 3072, 4096], P(None, 'dp', ('fsdp', 'mp'))
- loss: float32 [16384], P(('dp', 'fsdp', 'mp'))
The draws below stay inside these ranges and needn't reach their ends.
Inputs may be any that keep to these rules, and one draw needn't show every extreme that they name: `old_block`: a permutation of the old layout's row blocks. `new_residue`: a permutation; index i of dp holds the rows whose number modulo 8 is new_residue[i], in rising order. `segment_ids`: never falling along the tokens.
All inputs are finite; a program needn't handle non-finite values.
Results may differ from the reference program's by a relative error of at most 0.0075.
Values may be sent and summed in bfloat16 or wider, within the bound.
A program may use at most 192 MiB of HBM per device.

```python
import math
import jax
import jax.numpy as jnp
import numpy as np
from jax import lax

D = 3072
HD = 128
HF = 4096
VOC = 16384
SEQ = 2048
TOKENS = 16384
N_DP = 8
N_FSDP = 8
N_MP = 2
DEVICES = 128


def draw_tokens_in(key, part):
    keys = jax.random.split(key, 1)
    drawn = jnp.clip(jax.random.normal(keys[0], (TOKENS, D), jnp.float32), -6.0, 6.0)
    return jnp.clip(drawn, -40.0, 40.0).astype(jnp.bfloat16)


def draw_old_weights(key, part):
    raw = jnp.clip(jax.random.normal(key, (4, D, HF), jnp.float32), -6.0, 6.0)
    fan_width = jnp.array([D, D, D, HF], jnp.float32).reshape(4, 1, 1)
    scaled = raw / jnp.sqrt(fan_width)
    return scaled.astype(jnp.bfloat16)


def draw_head_weight(key, part):
    keys = jax.random.split(key, 1)
    raw = jnp.clip(jax.random.normal(keys[0], (D, VOC), jnp.float32), -6.0, 6.0) / math.sqrt(D)
    return raw.astype(jnp.bfloat16)


def plant(result, own_key, least, largest):
    extent = result.shape
    index_at = [jax.random.randint(jax.random.fold_in(own_key, axis), (), 0, extent[axis]) for axis in range(len(extent))]
    result = result.at[tuple(index_at)].set(least)
    longest = extent.index(max(extent))
    index_at[longest] = (index_at[longest] + 1) % extent[longest]
    return result.at[tuple(index_at)].set(largest)


def levels(key, extent, cuts, low, top_value):
    def one(dim, shards_of):
        steps = jax.random.uniform(jax.random.fold_in(jax.random.fold_in(key, 6), dim), (shards_of,), jnp.float32, low / len(cuts), top_value / len(cuts))
        return jnp.repeat(jnp.exp(steps), extent[dim] // shards_of).reshape((-1,) + (1,) * (len(extent) - dim - 1))

    level = one(*cuts[0])
    for cut in cuts[1:]:
        level = level * one(*cut)
    return level


def rank_table(number_of, lean):
    loads = [(1 << 20) // math.isqrt(standing ** lean) + 1 for standing in range(1, number_of + 1)]
    deviation = 1 + sum(loads) // (1 << 30)
    return np.cumsum(np.array([max(1, weight // deviation) for weight in loads]))


def ranked(rng, dims, amount, slope):
    grid = rank_table(amount, slope)
    lot = jax.random.randint(jax.random.fold_in(rng, 1), dims, 0, int(grid[amount - 1]))
    grade = jnp.searchsorted(jnp.asarray(grid, jnp.int32), lot, side="right")
    return jax.random.permutation(jax.random.fold_in(rng, 2), amount)[grade].astype(jnp.int32)


def profile(number_of, total, bound, lean):
    loads = [(1 << 20) // math.isqrt(rank ** lean) + 1 for rank in range(2, number_of + 1)]
    spare, given = total - bound - (number_of - 1), [1] * (number_of - 1)
    while spare > 0:
        candidates = [i for i in range(number_of - 1) if given[i] < bound]
        pool, remaining = sum([loads[i] for i in candidates]), spare
        for i in candidates:
            addition = min(bound - given[i], max(1, remaining * loads[i] // pool), spare)
            given[i] = given[i] + addition
            spare = spare - addition
    return np.array([bound] + given)


def ragged(key, amount, total, reach, slope):
    if amount == 2:
        one = jax.random.randint(key, (), max(1, total - reach), min(reach, total - 1) + 1)
        return jnp.stack([one, total - one])
    lengths = jnp.asarray(profile(amount, total, reach, slope), jnp.int32)
    pairs = (amount - 1) // 2
    source_of, sink = lengths[1:1 + 2 * pairs:2], lengths[2:2 + 2 * pairs:2]
    margin = jnp.minimum(source_of - 1, reach - sink)
    moved = jax.random.randint(jax.random.fold_in(key, 1), (pairs,), 0, 1 << 20) % (margin + 1)
    lengths = lengths.at[1:1 + 2 * pairs:2].set(source_of - moved).at[2:2 + 2 * pairs:2].set(sink + moved)
    return lengths[jax.random.permutation(jax.random.fold_in(key, 2), amount)]


def centred(own_key, dims, spread, most, cuts=(), kind=jnp.bfloat16):
    values = jax.random.normal(own_key, dims, jnp.float32) * spread
    if len(cuts) > 0:
        values = levels(own_key, dims, cuts, -0.22, 0.18) * values
    return jnp.clip(values, min=-most, max=most).astype(kind)


def setup_inputs(seed: int = 0) -> dict:
    arg_keys = jax.random.split(jax.random.key(seed), 11)
    return {
        "tokens_in": draw_tokens_in(jax.random.fold_in(arg_keys[10], 71), 0),
        "segment_ids": jnp.searchsorted(jnp.cumsum(ragged(arg_keys[1], 8 * N_DP, TOKENS, SEQ // 2, 2)), jnp.arange(TOKENS), side="right").astype(jnp.int32),
        "target_ids": plant(ranked(arg_keys[2], (TOKENS,), VOC, 2), jax.random.fold_in(arg_keys[2], 3), 0, VOC - 1).astype(jnp.int32),
        "old_weights": draw_old_weights(jax.random.fold_in(arg_keys[10], 71), 0),
        "old_first": centred(arg_keys[4], (4, D, HF), 1.0, 6.0, ((1, 128),), jnp.float32),
        "old_second": jnp.clip(jnp.exp(math.log(4.0) - 5.9914646 * jax.random.uniform(arg_keys[5], (4, D, HF), jnp.float32) ** levels(arg_keys[5], (4, D, HF), ((1, 128),), -0.2, 0.2)), 0.01, 4.0),
        "old_block": jax.random.permutation(arg_keys[6], DEVICES).astype(jnp.int32),
        "new_residue": jax.random.permutation(arg_keys[7], N_DP).astype(jnp.int32),
        "norm_gain": jnp.clip(1.0 + 0.1 * jax.random.normal(arg_keys[8], (D,), jnp.float32), 0.5, 1.5),
        "head_weight": draw_head_weight(jax.random.fold_in(arg_keys[10], 71), 0),
    }


def inverse_table(table):
    total_count = table.shape[0]
    return jnp.zeros((total_count,), jnp.int32).at[table].set(jnp.arange(total_count, dtype=jnp.int32))

def logical_rows(stored, holder):
    matrices, row_count, columns = stored.shape
    devices = holder.shape[0]
    split_rows = stored.reshape(matrices, devices, row_count // devices, columns)
    return jnp.take(split_rows, holder, axis=1).reshape(matrices, row_count, columns)

def new_layout(logical, new_residue):
    matrices, row_count, columns = logical.shape
    dp_count = new_residue.shape[0]
    picked = jnp.take(logical.reshape(matrices, row_count // dp_count, dp_count, columns), new_residue, axis=2)
    return picked.transpose(0, 2, 1, 3).reshape(matrices, row_count, columns)

def one_sequence(tokens, segments, targets, weights, norm_gain, head_weight):
    seq_len = tokens.shape[0]
    columns = weights.shape[2]
    heads = columns // HD
    groups = N_FSDP * N_MP
    group_cols = columns // groups
    queries = jnp.dot(tokens, weights[0], preferred_element_type=jnp.float32).astype(jnp.bfloat16)
    keys_all = jnp.dot(tokens, weights[1], preferred_element_type=jnp.float32).astype(jnp.bfloat16)
    values_all = jnp.dot(tokens, weights[2], preferred_element_type=jnp.float32).astype(jnp.bfloat16)
    queries = queries.reshape(seq_len, heads, HD).astype(jnp.float32)
    keys_all = keys_all.reshape(seq_len, heads, HD).astype(jnp.float32)
    values_all = values_all.reshape(seq_len, heads, HD).astype(jnp.float32)
    positions = jnp.arange(seq_len, dtype=jnp.int32)
    allowed = (positions[:, None] >= positions[None, :]) & (segments[:, None] == segments[None, :])
    scores = jnp.einsum('shd,thd->hst', queries, keys_all) * (1.0 / math.sqrt(HD))
    scores = jnp.where(allowed[None], scores, -1e+30)
    row_max = lax.optimization_barrier(jnp.max(scores, axis=2, keepdims=True))
    expo = jnp.where(allowed[None], jnp.exp(scores - row_max), 0.0)
    soft = (expo / lax.optimization_barrier(jnp.sum(expo, axis=2, keepdims=True))).astype(jnp.bfloat16)
    attended = jnp.einsum('hst,thd->shd', soft.astype(jnp.float32), values_all).astype(jnp.bfloat16)
    attended = attended.reshape(seq_len, groups, group_cols).astype(jnp.float32)
    out_proj = weights[3].reshape(-1, groups, group_cols).astype(jnp.float32)
    parts = jnp.einsum('sgc,dgc->gsd', attended, out_proj).astype(jnp.bfloat16)
    parts = lax.optimization_barrier(parts)
    summed = lax.optimization_barrier(jnp.sum(parts.astype(jnp.float32), axis=0))
    hidden = tokens.astype(jnp.float32) + summed
    scale = lax.rsqrt(lax.optimization_barrier(jnp.mean(hidden * hidden, axis=1, keepdims=True)) + 1e-05)
    normed = (hidden * scale * norm_gain).astype(jnp.bfloat16)
    logits = jnp.dot(normed, head_weight, preferred_element_type=jnp.float32)
    row_top = lax.optimization_barrier(jnp.max(logits, axis=1))
    row_total = lax.optimization_barrier(jnp.sum(jnp.exp(logits - row_top[:, None]), axis=1))
    vocab_ids = jnp.arange(logits.shape[1], dtype=jnp.int32)
    picked = lax.optimization_barrier(jnp.sum(jnp.where(vocab_ids[None, :] == targets[:, None], logits, 0.0), axis=1))
    return row_top + jnp.log(row_total) - picked

def reference(tokens_in, segment_ids, target_ids, old_weights, old_first, old_second, old_block, new_residue, norm_gain, head_weight):
    holder = inverse_table(old_block)
    weights = logical_rows(old_weights, holder)
    new_weights = new_layout(weights, new_residue)
    new_first = new_layout(logical_rows(old_first, holder), new_residue)
    new_second = new_layout(logical_rows(old_second, holder), new_residue)
    seq_tokens = tokens_in.reshape(N_DP, SEQ, D)
    seq_segments = segment_ids.reshape(N_DP, SEQ)
    seq_targets = target_ids.reshape(N_DP, SEQ)

    def per_sequence(packed):
        return one_sequence(packed[0], packed[1], packed[2], weights, norm_gain, head_weight)
    losses = lax.map(per_sequence, (seq_tokens, seq_segments, seq_targets))
    return (new_weights, new_first, new_second, losses.reshape(TOKENS))
```

```python
import functools
import math

import jax
import jax.numpy as jnp
from jax import lax
from jax.experimental import pallas as pl
from jax.experimental.pallas import tpu as pltpu
from jax.sharding import PartitionSpec as P

HD = 128
MESH = pl.DeviceIdType.MESH
A_END, A_MID, B_MID = 48, 32, 80
VMEM = pl.BlockSpec(memory_space=pltpu.VMEM)
ANY = pl.BlockSpec(memory_space=pl.ANY)


class Place:
    def __init__(self):
        self.dp = lax.axis_index("dp")
        self.fs = lax.axis_index("fsdp")
        self.g = lax.axis_index("mp")
        self.x, self.c = lax.div(self.dp, 2), lax.rem(self.dp, 2)
        self.zl, self.y = lax.div(self.fs, 4), lax.rem(self.fs, 4)
        self.fm = self.fs * 2 + self.g
        self.n = lax.rem(self.c + self.g, 2)

    def flip_z(self, rz):
        return 1 - self.zl if rz else self.zl

    def turn_y(self, ry):
        return lax.rem(self.y + ry, 4)

    def slot(self, rz, ry):
        z = self.flip_z(rz)
        return (z + self.n - 2 * z * self.n) * 8 + self.turn_y(ry) * 2 + self.c

    def other_slot(self, rz, ry):
        z, n = self.flip_z(rz), 1 - self.n
        return (z + n - 2 * z * n) * 8 + self.turn_y(ry) * 2 + 1 - self.c

    def at(self, rx=0, rz=0, ry=0):
        return (
            lax.rem(self.x + rx, 4) * 2 + self.c,
            self.flip_z(rz) * 4 + self.turn_y(ry),
            self.g,
        )

    def twin(self):
        return (self.x * 2 + 1 - self.c, self.fs, self.g)

    def across(self, core):
        return (self.x * 2 + core, (1 - self.zl) * 4 + self.y, 1 - self.g)


class Sends:
    def __init__(self, send_sem, recv_sem):
        self.send_sem, self.recv_sem, self.count, self.open = send_sem, recv_sem, 0, []

    def make(self, src, dst, device):
        k = self.count
        self.count += 1
        return pltpu.make_async_remote_copy(
            src_ref=src,
            dst_ref=dst,
            send_sem=self.send_sem.at[k],
            recv_sem=self.recv_sem.at[k],
            device_id=device,
            device_id_type=MESH,
        )

    def start(self, src, dst, device):
        copy = self.make(src, dst, device)
        copy.start()
        self.open.append(copy)
        return copy

    def finish(self):
        for copy in self.open:
            copy.wait_send()


def greet(devices):
    barrier = pltpu.get_barrier_semaphore()
    for device in devices:
        pl.semaphore_signal(barrier, inc=1, device_id=device, device_id_type=MESH)
    pl.semaphore_wait(barrier, len(devices))


class BlockGather:
    def __init__(self, me, full, sends):
        self.me, self.full, self.sends, self.got, self.twins = me, full, sends, {}, []

    def send(self, key, rz, ry, start, end, device):
        part = self.full.at[self.me.slot(rz, ry), pl.ds(start, end - start)]
        self.got[key] = self.sends.start(part, part, device)

    def wait(self, *keys):
        for key in keys:
            self.got[key].wait_recv()

    def share(self, rz, ry):
        block = self.full.at[self.me.slot(rz, ry)]
        self.twins.append(self.sends.start(block, block, self.me.twin()))

    def first(self):
        me = self.me
        self.up, self.down, self.over = me.at(ry=1), me.at(ry=3), me.at(rz=1)
        self.send("ay0", 0, 0, 0, A_END, self.up)
        self.send("ay1", 0, 0, 0, A_END, self.down)
        self.send("bz", 0, 0, A_END, 128, self.over)
        self.send("az0", 0, 0, 0, A_END, self.over)
        self.send("by0", 0, 0, A_END, 128, self.up)
        self.send("by1", 0, 0, A_END, 128, self.down)
        self.share(0, 0)

    def second(self):
        self.wait("ay0")
        self.send("af0", 0, 3, 0, A_MID, self.up)
        self.send("az3", 0, 3, 0, A_END, self.over)
        self.wait("ay1")
        self.send("af1", 0, 1, A_MID, A_END, self.down)
        self.send("az1", 0, 1, 0, A_END, self.over)
        self.wait("bz")
        self.send("by2", 1, 0, A_END, 128, self.up)
        self.send("by3", 1, 0, A_END, 128, self.down)

    def third(self):
        self.wait("af0", "af1")
        self.send("az2", 0, 2, 0, A_END, self.over)
        self.wait("by0")
        self.send("bf0", 0, 3, A_END, B_MID, self.up)
        self.wait("by1")
        self.send("bf1", 0, 1, B_MID, 128, self.down)
        self.share(0, 1)
        self.share(0, 3)
        self.wait("az0")
        self.share(1, 0)

    def fourth(self):
        self.wait("by2")
        self.send("bf2", 1, 3, A_END, B_MID, self.up)
        self.wait("by3")
        self.send("bf3", 1, 1, B_MID, 128, self.down)
        self.wait("az3", "az1")
        self.share(1, 1)
        self.share(1, 3)

    def last(self):
        self.wait("bf0", "bf1")
        self.share(0, 2)
        self.wait("az2", "bf2", "bf3")
        self.share(1, 2)
        for copy in self.twins:
            copy.wait_recv()


def gather_kernel(
    tok,
    small,
    wpk,
    xfull,
    sfull,
    wfull,
    wown,
    send_sem,
    recv_sem,
    local_sem,
    ex_send,
    ex_recv,
    small_send,
    small_recv,
):
    me = Place()
    sends = Sends(send_sem, recv_sem)
    mine = me.c * 16 + me.fm

    barrier = pltpu.get_barrier_semaphore()

    @pl.loop(1, 32)
    def _(k):
        q = lax.rem(mine + k, 32)
        fm = lax.rem(q, 16)
        device = (me.x * 2 + lax.div(q, 16), lax.div(fm, 2), lax.rem(fm, 2))
        pl.semaphore_signal(barrier, inc=1, device_id=device, device_id_type=MESH)

    for rx in (1, 3):
        pl.semaphore_signal(barrier, inc=1, device_id=me.at(rx=rx), device_id_type=MESH)
    pl.semaphore_wait(barrier, 33)

    keep = pltpu.make_async_copy(tok, xfull.at[me.fm], local_sem.at[0])
    swap = sends.make(tok, xfull.at[me.fm], me.across(1 - me.c))

    @pl.when(me.n == 0)
    def _():
        keep.start()

    @pl.when(me.n == 1)
    def _():
        swap.start()

    def exchange(k):
        t = lax.rem(me.fm + k, 16)
        return pltpu.make_async_remote_copy(
            src_ref=wpk.at[t],
            dst_ref=wown.at[me.fm],
            send_sem=ex_send.at[k],
            recv_sem=ex_recv.at[k],
            device_id=(me.dp, lax.div(t, 2), lax.rem(t, 2)),
            device_id_type=MESH,
        )

    @pl.loop(1, 16)
    def _(k):
        exchange(k).start()

    own = pltpu.make_async_copy(wpk.at[me.fm], wown.at[me.fm], local_sem.at[1])
    own.start()

    def tell(k):
        q = lax.rem(me.c * 8 + me.fs + k, 16)
        return pltpu.make_async_remote_copy(
            src_ref=small,
            dst_ref=sfull.at[me.fm],
            send_sem=small_send.at[k],
            recv_sem=small_recv.at[me.fm],
            device_id=(me.x * 2 + lax.div(q, 8), lax.rem(q, 8), me.c),
            device_id_type=MESH,
        )

    note = pltpu.make_async_copy(small, sfull.at[me.fm], local_sem.at[2])

    @pl.when(me.n == 1)
    def _():
        tell(0).start()

    @pl.when(me.n == 0)
    def _():
        note.start()

    @pl.loop(1, 16)
    def _(k):
        tell(k).start()

    @pl.when(me.n == 0)
    def _():
        keep.wait()

    @pl.when(me.n == 1)
    def _():
        swap.wait_recv()

    blocks = BlockGather(me, xfull, sends)
    blocks.first()

    own.wait()

    @pl.loop(1, 16)
    def _(k):
        exchange(k).wait_recv()

    far = pltpu.make_async_remote_copy(
        src_ref=wown,
        dst_ref=wfull.at[me.dp],
        send_sem=ex_send.at[16],
        recv_sem=ex_recv.at[16 + me.c],
        device_id=me.across(me.g),
        device_id_type=MESH,
    )
    far.start()
    near = pltpu.make_async_remote_copy(
        src_ref=wown,
        dst_ref=wfull.at[me.dp],
        send_sem=ex_send.at[17],
        recv_sem=ex_recv.at[18],
        device_id=me.twin(),
        device_id_type=MESH,
    )
    stay = pltpu.make_async_copy(wown, wfull.at[me.dp], local_sem.at[3])

    @pl.when(me.n == 1)
    def _():
        near.start()

    @pl.when(me.n == 0)
    def _():
        stay.start()

    blocks.second()

    def from_core(core):
        return pltpu.make_async_remote_copy(
            src_ref=wown,
            dst_ref=wfull.at[me.dp],
            send_sem=ex_send.at[16],
            recv_sem=ex_recv.at[16 + core],
            device_id=me.across(me.g),
            device_id_type=MESH,
        )

    @pl.when(me.n == 1)
    def _():
        from_core(0).wait_recv()
        from_core(1).wait_recv()

    @pl.when(me.n == 0)
    def _():
        near.wait_recv()
        stay.wait()

    right, left = me.at(rx=1), me.at(rx=3)
    pair = wfull.at[pl.ds(me.x * 2, 2)]
    to_right = sends.start(pair, pair, right)
    to_left = sends.start(pair, pair, left)
    blocks.third()
    blocks.fourth()
    to_right.wait_recv()
    first = wfull.at[lax.rem(me.x + 3, 4) * 2]
    on_right = sends.start(first, first, right)
    to_left.wait_recv()
    second = wfull.at[lax.rem(me.x + 1, 4) * 2 + 1]
    on_left = sends.start(second, second, left)
    blocks.last()
    on_right.wait_recv()
    on_left.wait_recv()

    @pl.loop(0, 16)
    def _(j):
        @pl.when(jnp.logical_or(me.n == 1, j != me.fm))
        def _():
            pltpu.make_async_remote_copy(
                src_ref=small,
                dst_ref=sfull.at[j],
                send_sem=small_send.at[0],
                recv_sem=small_recv.at[j],
                device_id=me.twin(),
                device_id_type=MESH,
            ).wait_recv()

    @pl.loop(1, 16)
    def _(k):
        exchange(k).wait_send()
        tell(k).wait_send()

    far.wait_send()

    @pl.when(me.n == 1)
    def _():
        tell(0).wait_send()
        near.wait_send()
        swap.wait_send()

    @pl.when(me.n == 0)
    def _():
        note.wait()

    sends.finish()


def params(collective_id):
    return pltpu.CompilerParams(
        collective_id=collective_id, has_side_effects=True, vmem_limit_bytes=60 * 2**20
    )


def gather_inputs(tokens, small, wpk):
    rows, width = tokens.shape
    return pl.pallas_call(
        gather_kernel,
        name="gather_inputs",
        out_shape=(
            jax.ShapeDtypeStruct((16, rows, width), tokens.dtype),
            jax.ShapeDtypeStruct((16, *small.shape), small.dtype),
            jax.ShapeDtypeStruct((8, *wpk.shape), wpk.dtype),
        ),
        in_specs=[VMEM] * 3,
        out_specs=(ANY, VMEM, ANY),
        scratch_shapes=[
            pltpu.VMEM(wpk.shape, wpk.dtype),
            pltpu.SemaphoreType.DMA((40,)),
            pltpu.SemaphoreType.DMA((40,)),
            pltpu.SemaphoreType.DMA((4,)),
            pltpu.SemaphoreType.DMA((18,)),
            pltpu.SemaphoreType.DMA((19,)),
            pltpu.SemaphoreType.DMA((16,)),
            pltpu.SemaphoreType.DMA((16,)),
        ],
        compiler_params=params(0),
    )(tokens, small, wpk)


def gather_normed_kernel(block, full, send_sem, recv_sem, local_sem):
    me = Place()
    sends = Sends(send_sem, recv_sem)
    greet([me.at(ry=1), me.at(ry=3), me.at(rz=1), me.twin()])
    keep = pltpu.make_async_copy(block, full.at[me.slot(0, 0)], local_sem.at[0])
    keep.start()
    keep.wait()
    blocks = BlockGather(me, full, sends)
    blocks.first()
    blocks.second()
    blocks.third()
    blocks.fourth()
    blocks.last()
    sends.finish()


def gather_normed(block):
    return pl.pallas_call(
        gather_normed_kernel,
        name="gather_normed",
        out_shape=jax.ShapeDtypeStruct((16, *block.shape), block.dtype),
        in_specs=[VMEM],
        out_specs=ANY,
        scratch_shapes=[
            pltpu.SemaphoreType.DMA((32,)),
            pltpu.SemaphoreType.DMA((32,)),
            pltpu.SemaphoreType.DMA((1,)),
        ],
        compiler_params=params(1),
    )(block)


def add_rows(into, start, end, *others):
    @pl.loop(0, (end - start) // 16)
    def _(i):
        rows = pl.ds(pl.multiple_of(start + i * 16, 16), 16)
        total = into[rows].astype(jnp.float32)
        for other in others:
            total += other[pl.ds(pl.multiple_of(i * 16, 16), 16)].astype(jnp.float32)
        into[rows] = total.astype(into.dtype)


def scatter_kernel(
    part, hw, out, hwx, r, za, zb, fa0, fa1, ya, fb0, fb1, yb, send_sem, recv_sem, local_sem, hs, hr
):
    me = Place()
    sends = Sends(send_sem, recv_sem)
    up, down, over, twin = me.at(ry=1), me.at(ry=3), me.at(rz=1), me.twin()
    right, left, partner = me.at(rx=1), me.at(rx=3), me.across(me.c)
    greet([up, down, over, twin, right, left, partner])

    order = [(1, 2), (1, 0), (1, 1), (1, 3), (0, 2), (0, 1), (0, 3), (0, 0)]
    halves = [
        sends.start(part.at[me.other_slot(rz, ry)], r.at[rz * 4 + ry], twin) for rz, ry in order
    ]

    quarter = hw.shape[0] // 4
    half = quarter // 2

    def head_copy(k, start, size, device, src):
        rows = pl.ds(start, size)
        return pltpu.make_async_remote_copy(
            src_ref=src.at[rows],
            dst_ref=hwx.at[rows],
            send_sem=hs.at[k],
            recv_sem=hr.at[k],
            device_id=device,
            device_id_type=MESH,
        )

    head_out = head_copy(0, me.x * quarter, quarter, partner, hw)
    head_keep = pltpu.make_async_copy(hw, hwx, local_sem.at[0])
    head_right = head_copy(1, me.x * quarter, quarter, right, hwx)
    head_left = head_copy(2, me.x * quarter, quarter, left, hwx)
    head_right2 = head_copy(3, lax.rem(me.x + 3, 4) * quarter, half, right, hwx)
    head_left2 = head_copy(4, lax.rem(me.x + 1, 4) * quarter + half, half, left, hwx)

    @pl.when(me.n == 0)
    def _():
        head_out.start()
        head_keep.start()

    a_got, b_got, y_got = {}, {}, {}
    for (rz, ry), copy in zip(order, halves):
        copy.wait_recv()
        block = r.at[rz * 4 + ry]
        add_rows(block, 0, 128, part.at[me.slot(rz, ry)])
        if rz == 1:
            a_got[ry] = sends.start(block.at[pl.ds(0, A_END)], za.at[ry], over)
        if ry == 2:
            b_got[rz, 0] = sends.start(block.at[pl.ds(A_END, B_MID - A_END)], fb0.at[rz], up)
            b_got[rz, 1] = sends.start(block.at[pl.ds(B_MID, 128 - B_MID)], fb1.at[rz], down)

    @pl.when(me.n == 1)
    def _():
        head_out.wait_recv()
        head_right.start()
        head_left.start()

    tail = pl.ds(A_END, 128 - A_END)
    for rz in (1, 0):
        b_got[rz, 0].wait_recv()
        add_rows(r.at[rz * 4 + 1], A_END, B_MID, fb0.at[rz])
        y_got[rz, 0] = sends.start(r.at[rz * 4 + 1, tail], yb.at[rz * 2], up)
        b_got[rz, 1].wait_recv()
        add_rows(r.at[rz * 4 + 3], B_MID, 128, fb1.at[rz])
        y_got[rz, 1] = sends.start(r.at[rz * 4 + 3, tail], yb.at[rz * 2 + 1], down)

    head = pl.ds(0, A_END)
    a_got[2].wait_recv()
    add_rows(r.at[2], 0, A_END, za.at[2])
    f_up = sends.start(r.at[2, pl.ds(0, A_MID)], fa0, up)
    f_down = sends.start(r.at[2, pl.ds(A_MID, A_END - A_MID)], fa1, down)

    y_got[1, 0].wait_recv()
    y_got[1, 1].wait_recv()
    add_rows(r.at[4], A_END, 128, yb.at[2], yb.at[3])
    z_got = sends.start(r.at[4, tail], zb, over)

    @pl.when(me.n == 1)
    def _():
        head_right.wait_recv()
        head_right2.start()
        head_left.wait_recv()
        head_left2.start()

    a_got[1].wait_recv()
    add_rows(r.at[1], 0, A_END, za.at[1])
    f_up.wait_recv()
    add_rows(r.at[1], 0, A_MID, fa0)
    g_up = sends.start(r.at[1, head], ya.at[0], up)
    a_got[3].wait_recv()
    add_rows(r.at[3], 0, A_END, za.at[3])
    f_down.wait_recv()
    add_rows(r.at[3], A_MID, A_END, fa1)
    g_down = sends.start(r.at[3, head], ya.at[1], down)

    def total(start, end, others):
        @pl.loop(0, (end - start) // 16)
        def _(i):
            here = pl.ds(pl.multiple_of(i * 16, 16), 16)
            rows = pl.ds(pl.multiple_of(start + i * 16, 16), 16)
            value = r[0, rows].astype(jnp.float32)
            for other in others:
                value += other[here].astype(jnp.float32)
            out[rows] = value

    y_got[0, 0].wait_recv()
    y_got[0, 1].wait_recv()
    z_got.wait_recv()
    total(A_END, 128, [yb.at[0], yb.at[1], zb])
    a_got[0].wait_recv()
    g_up.wait_recv()
    g_down.wait_recv()
    total(0, A_END, [za.at[0], ya.at[0], ya.at[1]])

    @pl.when(me.n == 1)
    def _():
        head_right2.wait_recv()
        head_left2.wait_recv()
        head_right.wait_send()
        head_left.wait_send()
        head_right2.wait_send()
        head_left2.wait_send()

    @pl.when(me.n == 0)
    def _():
        head_out.wait_send()
        head_keep.wait()

    sends.finish()


def scatter_parts(part, hw):
    blocks, rows, width = part.shape
    dtype = part.dtype
    return pl.pallas_call(
        scatter_kernel,
        name="scatter_parts",
        out_shape=(
            jax.ShapeDtypeStruct((rows, width), jnp.float32),
            jax.ShapeDtypeStruct(hw.shape, hw.dtype),
        ),
        in_specs=[VMEM, ANY],
        out_specs=(VMEM, ANY),
        scratch_shapes=[
            pltpu.VMEM((8, rows, width), dtype),
            pltpu.VMEM((4, A_END, width), dtype),
            pltpu.VMEM((rows - A_END, width), dtype),
            pltpu.VMEM((A_MID, width), dtype),
            pltpu.VMEM((A_END - A_MID, width), dtype),
            pltpu.VMEM((2, A_END, width), dtype),
            pltpu.VMEM((2, B_MID - A_END, width), dtype),
            pltpu.VMEM((2, rows - B_MID, width), dtype),
            pltpu.VMEM((4, rows - A_END, width), dtype),
            pltpu.SemaphoreType.DMA((32,)),
            pltpu.SemaphoreType.DMA((32,)),
            pltpu.SemaphoreType.DMA((1,)),
            pltpu.SemaphoreType.DMA((5,)),
            pltpu.SemaphoreType.DMA((5,)),
        ],
        compiler_params=params(2),
    )(part, hw)


def totals_kernel(stats, got, send_sem, recv_sem, local_sem):
    me = Place()
    barrier = pltpu.get_barrier_semaphore()
    mine = me.c * 16 + me.fm

    @pl.loop(1, 32)
    def _(k):
        q = lax.rem(mine + k, 32)
        fm = lax.rem(q, 16)
        device = (me.x * 2 + lax.div(q, 16), lax.div(fm, 2), lax.rem(fm, 2))
        pl.semaphore_signal(barrier, inc=1, device_id=device, device_id_type=MESH)

    pl.semaphore_wait(barrier, 31)
    sender = me.c * 8 + me.fs

    def tell(k):
        b = lax.rem(me.fm + k, 16)
        return pltpu.make_async_remote_copy(
            src_ref=stats.at[b],
            dst_ref=got.at[sender],
            send_sem=send_sem.at[k],
            recv_sem=recv_sem.at[sender],
            device_id=(me.x * 2 + me.g, lax.div(b, 2), lax.rem(b, 2)),
            device_id_type=MESH,
        )

    note = pltpu.make_async_copy(stats.at[me.fm], got.at[sender], local_sem.at[0])

    @pl.when(me.n == 1)
    def _():
        tell(0).start()

    @pl.when(me.n == 0)
    def _():
        note.start()

    @pl.loop(1, 16)
    def _(k):
        tell(k).start()

    @pl.loop(0, 16)
    def _(j):
        @pl.when(jnp.logical_or(me.n == 1, j != sender))
        def _():
            pltpu.make_async_remote_copy(
                src_ref=stats.at[0],
                dst_ref=got.at[j],
                send_sem=send_sem.at[0],
                recv_sem=recv_sem.at[j],
                device_id=me.twin(),
                device_id_type=MESH,
            ).wait_recv()

    @pl.loop(1, 16)
    def _(k):
        tell(k).wait_send()

    @pl.when(me.n == 1)
    def _():
        tell(0).wait_send()

    @pl.when(me.n == 0)
    def _():
        note.wait()


def exchange_totals(stats):
    return pl.pallas_call(
        totals_kernel,
        name="exchange_totals",
        out_shape=jax.ShapeDtypeStruct(stats.shape, stats.dtype),
        in_specs=[VMEM],
        out_specs=VMEM,
        scratch_shapes=[
            pltpu.SemaphoreType.DMA((16,)),
            pltpu.SemaphoreType.DMA((16,)),
            pltpu.SemaphoreType.DMA((1,)),
        ],
        compiler_params=params(3),
    )(stats)


def copy_for_each(value, axis):
    copies = jnp.broadcast_to(value, (lax.axis_size(axis), *value.shape))
    return lax.all_to_all(copies, axis, split_axis=0, concat_axis=0, tiled=True)


def inverse_of(table):
    total_count = table.shape[0]
    places = jnp.arange(total_count, dtype=jnp.int32)
    return jnp.sum(jnp.where(table[None, :] == places[:, None], places[None, :], 0), axis=1)


def pack_rows(stored, residues, fm_count):
    matrices, row_count, columns = stored.shape
    dp_count = residues.shape[0]
    split_rows = stored.reshape(
        matrices, row_count // dp_count, dp_count, fm_count, columns // fm_count
    )
    chosen = jnp.take(split_rows, residues, axis=2)
    return chosen.transpose(2, 3, 0, 1, 4).reshape(
        dp_count * fm_count, matrices, row_count // dp_count, columns // fm_count
    )


def unpack_rows(received, holder):
    ordered = jnp.take(received, holder, axis=0)
    devices, matrices, pair_rows, group_cols = ordered.shape
    return ordered.transpose(1, 0, 2, 3).reshape(matrices, devices * pair_rows, group_cols)


def everywhere(value):
    return lax.all_to_all(value, ("dp", "fsdp", "mp"), split_axis=0, concat_axis=0, tiled=True)


def forward(tokens_in, segment_ids, target_ids, old_weights, old_block, norm_gain, head_weight):
    me = Place()
    matrices, old_rows, columns = old_weights.shape
    groups = 16
    group_cols = columns // groups
    model_width = tokens_in.shape[1]

    by_group = old_weights.reshape(matrices, old_rows, groups, group_cols).transpose(2, 0, 1, 3)
    by_group = by_group.reshape(groups, matrices * old_rows, group_cols)
    number = jnp.broadcast_to(old_block.astype(jnp.bfloat16)[:, None, None], (groups, 8, group_cols))
    wpk = jnp.concatenate([by_group, number], axis=1)
    small = jnp.stack([segment_ids, target_ids] + [segment_ids] * 6)
    xfull, sfull, wfull = gather_inputs(tokens_in, small, wpk)

    wfull = wfull.reshape(128, *wpk.shape[1:])
    holder = inverse_of(wfull[:, matrices * old_rows, 0].astype(jnp.int32))
    logical = (
        jnp.take(wfull, holder, axis=0)[:, : matrices * old_rows]
        .reshape(128, matrices, old_rows, group_cols)
        .transpose(1, 0, 2, 3)
        .reshape(matrices, model_width, group_cols)
    )
    whole_tokens = xfull.reshape(-1, model_width)
    segments = sfull[:, 0].reshape(-1)
    targets = sfull[:, 1].reshape(-1)
    seq_len = whole_tokens.shape[0]

    projected = jnp.einsum(
        "sd,mdc->msc", whole_tokens, logical[:3], preferred_element_type=jnp.float32
    )
    heads = group_cols // HD
    queries = projected[0].astype(jnp.bfloat16).reshape(seq_len, heads, HD)
    keys_all = projected[1].astype(jnp.bfloat16).reshape(seq_len, heads, HD)
    values_all = projected[2].astype(jnp.bfloat16).reshape(seq_len, heads, HD)
    positions_all = jnp.arange(seq_len, dtype=jnp.int32)
    allowed = (positions_all[:, None] >= positions_all[None, :]) & (
        segments[:, None] == segments[None, :]
    )
    scores = jnp.einsum("shd,thd->hst", queries, keys_all, preferred_element_type=jnp.float32) * (
        1.0 / math.sqrt(HD)
    )
    scores = jnp.where(allowed[None], scores, -1e30)
    row_max = jnp.max(scores, axis=2, keepdims=True)
    expo = jnp.where(allowed[None], jnp.exp(scores - row_max), 0.0)
    soft = (expo / jnp.sum(expo, axis=2, keepdims=True)).astype(jnp.bfloat16)
    attended = jnp.einsum("hst,thd->shd", soft, values_all, preferred_element_type=jnp.float32)
    attended = attended.astype(jnp.bfloat16).reshape(seq_len, group_cols)
    partial_value = jnp.einsum(
        "sc,dc->sd", attended, logical[3], preferred_element_type=jnp.float32
    )
    partial_value = partial_value.astype(jnp.bfloat16).reshape(16, 128, model_width)
    summed, heads_used = scatter_parts(partial_value, head_weight)

    own = me.slot(0, 0)
    hidden = lax.dynamic_index_in_dim(xfull, own, 0, keepdims=False).astype(jnp.float32) + summed
    scale = lax.rsqrt(jnp.mean(hidden * hidden, axis=1, keepdims=True) + 1e-05)
    normed = (hidden * scale * norm_gain).astype(jnp.bfloat16)
    nfull = gather_normed(normed).reshape(seq_len, model_width)

    logits = jnp.dot(nfull, heads_used, preferred_element_type=jnp.float32)
    vocab_dev = logits.shape[1]
    row_top = jnp.max(logits, axis=1)
    row_total = jnp.sum(jnp.exp(logits - row_top[:, None]), axis=1)
    vocab_ids = jnp.arange(vocab_dev, dtype=jnp.int32) + own * vocab_dev
    picked = jnp.sum(jnp.where(vocab_ids[None, :] == targets[:, None], logits, 0.0), axis=1)
    stats = jnp.stack([row_top, row_total, picked] + [picked] * 5).reshape(8, 16, 128)
    got = exchange_totals(stats.transpose(1, 0, 2))
    top = jnp.max(got[:, 0], axis=0)
    total = jnp.sum(got[:, 1] * jnp.exp(got[:, 0] - top), axis=0)
    loss = top + jnp.log(total) - jnp.sum(got[:, 2], axis=0)
    return loss, holder


def body(
    tokens_in,
    segment_ids,
    target_ids,
    old_weights,
    old_first,
    old_second,
    old_block,
    new_residue,
    norm_gain,
    head_weight,
):
    loss, holder = forward(
        tokens_in, segment_ids, target_ids, old_weights, old_block, norm_gain, head_weight
    )
    residues = copy_for_each(new_residue, "dp").reshape(-1)
    moments = jnp.concatenate(
        [pack_rows(old_first, residues, 16), pack_rows(old_second, residues, 16)], axis=1
    )
    got = everywhere(moments)
    new_first = unpack_rows(got[:, :4], holder)
    new_second = unpack_rows(got[:, 4:], holder)
    new_weights = unpack_rows(everywhere(pack_rows(old_weights, residues, 16)), holder)
    return (new_weights, new_first, new_second, loss)


def solution(mesh):
    placed = (
        P(("dp", "fsdp", "mp"), None),
        P(("dp", "fsdp", "mp")),
        P(("dp", "fsdp", "mp")),
        P(None, ("dp", "fsdp", "mp"), None),
        P(None, ("dp", "fsdp", "mp"), None),
        P(None, ("dp", "fsdp", "mp"), None),
        P(("dp", "fsdp", "mp")),
        P("dp"),
        P(),
        P(None, ("fsdp", "mp")),
    )
    return jax.shard_map(
        body,
        mesh=mesh,
        in_specs=placed,
        out_specs=(
            P(None, "dp", ("fsdp", "mp")),
            P(None, "dp", ("fsdp", "mp")),
            P(None, "dp", ("fsdp", "mp")),
            P(("dp", "fsdp", "mp")),
        ),
        check_vma=False,
    )
```

```python
import math

import jax
import jax.numpy as jnp
from jax import lax
from jax.experimental import pallas as pl
from jax.experimental.pallas import tpu as pltpu
from jax.sharding import PartitionSpec as P

HD = 128
MESH = pl.DeviceIdType.MESH
A_END, A_MID, B_MID = 48, 32, 80
VMEM = pl.BlockSpec(memory_space=pltpu.VMEM)
ANY = pl.BlockSpec(memory_space=pl.ANY)


class Place:
    def __init__(self):
        self.dp = lax.axis_index("dp")
        self.fs = lax.axis_index("fsdp")
        self.g = lax.axis_index("mp")
        self.x, self.c = lax.div(self.dp, 2), lax.rem(self.dp, 2)
        self.zl, self.y = lax.div(self.fs, 4), lax.rem(self.fs, 4)
        self.fm = self.fs * 2 + self.g
        self.n = lax.rem(self.c + self.g, 2)

    def flip_z(self, rz):
        return 1 - self.zl if rz else self.zl

    def turn_y(self, ry):
        return lax.rem(self.y + ry, 4)

    def slot(self, rz, ry):
        z = self.flip_z(rz)
        return (z + self.n - 2 * z * self.n) * 8 + self.turn_y(ry) * 2 + self.c

    def other_slot(self, rz, ry):
        z, n = self.flip_z(rz), 1 - self.n
        return (z + n - 2 * z * n) * 8 + self.turn_y(ry) * 2 + 1 - self.c

    def at(self, rx=0, rz=0, ry=0):
        return (
            lax.rem(self.x + rx, 4) * 2 + self.c,
            self.flip_z(rz) * 4 + self.turn_y(ry),
            self.g,
        )

    def twin(self):
        return (self.x * 2 + 1 - self.c, self.fs, self.g)

    def across(self, core):
        return (self.x * 2 + core, (1 - self.zl) * 4 + self.y, 1 - self.g)


class Sends:
    def __init__(self, send_sem, recv_sem):
        self.send_sem, self.recv_sem, self.count, self.open = send_sem, recv_sem, 0, []

    def make(self, src, dst, device):
        k = self.count
        self.count += 1
        return pltpu.make_async_remote_copy(
            src_ref=src,
            dst_ref=dst,
            send_sem=self.send_sem.at[k],
            recv_sem=self.recv_sem.at[k],
            device_id=device,
            device_id_type=MESH,
        )

    def start(self, src, dst, device):
        copy = self.make(src, dst, device)
        copy.start()
        self.open.append(copy)
        return copy

    def finish(self):
        for copy in self.open:
            copy.wait_send()


def greet(devices):
    barrier = pltpu.get_barrier_semaphore()
    for device in devices:
        pl.semaphore_signal(barrier, inc=1, device_id=device, device_id_type=MESH)
    pl.semaphore_wait(barrier, len(devices))


def greet_plane(me, extra=()):
    barrier = pltpu.get_barrier_semaphore()

    @pl.loop(1, 32)
    def _(k):
        q = lax.rem(me.c * 16 + me.fm + k, 32)
        fm = lax.rem(q, 16)
        device = (me.x * 2 + lax.div(q, 16), lax.div(fm, 2), lax.rem(fm, 2))
        pl.semaphore_signal(barrier, inc=1, device_id=device, device_id_type=MESH)

    for device in extra:
        pl.semaphore_signal(barrier, inc=1, device_id=device, device_id_type=MESH)
    pl.semaphore_wait(barrier, 31 + len(extra))


class BlockGather:
    def __init__(self, me, full, sends):
        self.me, self.full, self.sends, self.got, self.twins = me, full, sends, {}, []

    def send(self, key, rz, ry, start, end, device):
        part = self.full.at[self.me.slot(rz, ry), pl.ds(start, end - start)]
        self.got[key] = self.sends.start(part, part, device)

    def wait(self, *keys):
        for key in keys:
            self.got[key].wait_recv()

    def share(self, rz, ry):
        block = self.full.at[self.me.slot(rz, ry)]
        self.twins.append(self.sends.start(block, block, self.me.twin()))

    def first(self):
        me = self.me
        self.up, self.down, self.over = me.at(ry=1), me.at(ry=3), me.at(rz=1)
        self.send("ay0", 0, 0, 0, A_END, self.up)
        self.send("ay1", 0, 0, 0, A_END, self.down)
        self.send("bz", 0, 0, A_END, 128, self.over)
        self.send("az0", 0, 0, 0, A_END, self.over)
        self.send("by0", 0, 0, A_END, 128, self.up)
        self.send("by1", 0, 0, A_END, 128, self.down)
        self.share(0, 0)

    def second(self):
        self.wait("ay0")
        self.send("af0", 0, 3, 0, A_MID, self.up)
        self.send("az3", 0, 3, 0, A_END, self.over)
        self.wait("ay1")
        self.send("af1", 0, 1, A_MID, A_END, self.down)
        self.send("az1", 0, 1, 0, A_END, self.over)
        self.wait("bz")
        self.send("by2", 1, 0, A_END, 128, self.up)
        self.send("by3", 1, 0, A_END, 128, self.down)

    def third(self):
        self.wait("af0", "af1")
        self.send("az2", 0, 2, 0, A_END, self.over)
        self.wait("by0")
        self.send("bf0", 0, 3, A_END, B_MID, self.up)
        self.wait("by1")
        self.send("bf1", 0, 1, B_MID, 128, self.down)
        self.share(0, 1)
        self.share(0, 3)
        self.wait("az0")
        self.share(1, 0)

    def fourth(self):
        self.wait("by2")
        self.send("bf2", 1, 3, A_END, B_MID, self.up)
        self.wait("by3")
        self.send("bf3", 1, 1, B_MID, 128, self.down)
        self.wait("az3", "az1")
        self.share(1, 1)
        self.share(1, 3)

    def last(self):
        self.wait("bf0", "bf1")
        self.share(0, 2)
        self.wait("az2", "bf2", "bf3")
        self.share(1, 2)
        for copy in self.twins:
            copy.wait_recv()


def gather_kernel(
    holder,
    tok,
    small,
    wpk,
    xfull,
    sfull,
    wlog,
    wfull,
    wown,
    send_sem,
    recv_sem,
    local_sem,
    ex_send,
    ex_recv,
    small_send,
    small_recv,
):
    me = Place()
    sends = Sends(send_sem, recv_sem)
    greet_plane(me, [me.at(rx=1), me.at(rx=3)])

    keep = pltpu.make_async_copy(tok, xfull.at[me.fm], local_sem.at[0])
    swap = sends.make(tok, xfull.at[me.fm], me.across(1 - me.c))

    @pl.when(me.n == 0)
    def _():
        keep.start()

    @pl.when(me.n == 1)
    def _():
        swap.start()

    def exchange(k):
        t = lax.rem(me.fm + k, 16)
        return pltpu.make_async_remote_copy(
            src_ref=wpk.at[t],
            dst_ref=wown.at[me.fm],
            send_sem=ex_send.at[k],
            recv_sem=ex_recv.at[k],
            device_id=(me.dp, lax.div(t, 2), lax.rem(t, 2)),
            device_id_type=MESH,
        )

    @pl.loop(1, 16)
    def _(k):
        exchange(k).start()

    own = pltpu.make_async_copy(wpk.at[me.fm], wown.at[me.fm], local_sem.at[1])
    own.start()

    def tell(k):
        q = lax.rem(me.c * 8 + me.fs + k, 16)
        return pltpu.make_async_remote_copy(
            src_ref=small,
            dst_ref=sfull.at[me.fm],
            send_sem=small_send.at[k],
            recv_sem=small_recv.at[me.fm],
            device_id=(me.x * 2 + lax.div(q, 8), lax.rem(q, 8), me.c),
            device_id_type=MESH,
        )

    note = pltpu.make_async_copy(small, sfull.at[me.fm], local_sem.at[2])

    @pl.when(me.n == 1)
    def _():
        tell(0).start()

    @pl.when(me.n == 0)
    def _():
        note.start()

    @pl.loop(1, 16)
    def _(k):
        tell(k).start()

    @pl.when(me.n == 0)
    def _():
        keep.wait()

    @pl.when(me.n == 1)
    def _():
        swap.wait_recv()

    blocks = BlockGather(me, xfull, sends)
    blocks.first()

    own.wait()

    @pl.loop(1, 16)
    def _(k):
        exchange(k).wait_recv()

    far = pltpu.make_async_remote_copy(
        src_ref=wown,
        dst_ref=wfull.at[pl.ds(me.dp * 16, 16)],
        send_sem=ex_send.at[16],
        recv_sem=ex_recv.at[16 + me.c],
        device_id=me.across(me.g),
        device_id_type=MESH,
    )
    far.start()
    near = pltpu.make_async_remote_copy(
        src_ref=wown,
        dst_ref=wfull.at[pl.ds(me.dp * 16, 16)],
        send_sem=ex_send.at[17],
        recv_sem=ex_recv.at[18],
        device_id=me.twin(),
        device_id_type=MESH,
    )
    stay = pltpu.make_async_copy(wown, wfull.at[pl.ds(me.dp * 16, 16)], local_sem.at[3])

    @pl.when(me.n == 1)
    def _():
        near.start()

    @pl.when(me.n == 0)
    def _():
        stay.start()

    blocks.second()

    def from_core(core):
        return pltpu.make_async_remote_copy(
            src_ref=wown,
            dst_ref=wfull.at[pl.ds(me.dp * 16, 16)],
            send_sem=ex_send.at[16],
            recv_sem=ex_recv.at[16 + core],
            device_id=me.across(me.g),
            device_id_type=MESH,
        )

    @pl.when(me.n == 1)
    def _():
        from_core(0).wait_recv()
        from_core(1).wait_recv()

    @pl.when(me.n == 0)
    def _():
        near.wait_recv()
        stay.wait()

    right, left = me.at(rx=1), me.at(rx=3)
    pair = wfull.at[pl.ds(me.x * 32, 32)]
    to_right = sends.start(pair, pair, right)
    to_left = sends.start(pair, pair, left)
    blocks.third()
    blocks.fourth()
    to_right.wait_recv()
    first = wfull.at[pl.ds(lax.rem(me.x + 3, 4) * 32, 16)]
    on_right = sends.start(first, first, right)
    to_left.wait_recv()
    second = wfull.at[pl.ds(lax.rem(me.x + 1, 4) * 32 + 16, 16)]
    on_left = sends.start(second, second, left)
    blocks.last()
    on_right.wait_recv()
    on_left.wait_recv()

    rows = wpk.shape[1] // 4

    @pl.loop(0, 128)
    def _(b):
        where = holder[b]
        for m in range(4):
            wlog[m, pl.ds(pl.multiple_of(b * rows, 8), rows)] = wfull[
                where, pl.ds(m * rows, rows)
            ]

    @pl.loop(0, 16)
    def _(j):
        @pl.when(jnp.logical_or(me.n == 1, j != me.fm))
        def _():
            pltpu.make_async_remote_copy(
                src_ref=small,
                dst_ref=sfull.at[j],
                send_sem=small_send.at[0],
                recv_sem=small_recv.at[j],
                device_id=me.twin(),
                device_id_type=MESH,
            ).wait_recv()

    @pl.loop(1, 16)
    def _(k):
        exchange(k).wait_send()
        tell(k).wait_send()

    far.wait_send()

    @pl.when(me.n == 1)
    def _():
        tell(0).wait_send()
        near.wait_send()
        swap.wait_send()

    @pl.when(me.n == 0)
    def _():
        note.wait()

    sends.finish()


def params(collective_id):
    return pltpu.CompilerParams(
        collective_id=collective_id, has_side_effects=True, vmem_limit_bytes=60 * 2**20
    )


def gather_inputs(holder, tokens, small, wpk):
    rows, width = tokens.shape
    old_rows = wpk.shape[1] // 4
    return pl.pallas_call(
        gather_kernel,
        name="gather_inputs",
        out_shape=(
            jax.ShapeDtypeStruct((16, rows, width), tokens.dtype),
            jax.ShapeDtypeStruct((16, *small.shape), small.dtype),
            jax.ShapeDtypeStruct((4, 128 * old_rows, wpk.shape[2]), wpk.dtype),
        ),
        in_specs=[pl.BlockSpec(memory_space=pltpu.SMEM)] + [VMEM] * 3,
        out_specs=(ANY, VMEM, VMEM),
        scratch_shapes=[
            pltpu.VMEM((128, *wpk.shape[1:]), wpk.dtype),
            pltpu.VMEM(wpk.shape, wpk.dtype),
            pltpu.SemaphoreType.DMA((40,)),
            pltpu.SemaphoreType.DMA((40,)),
            pltpu.SemaphoreType.DMA((4,)),
            pltpu.SemaphoreType.DMA((18,)),
            pltpu.SemaphoreType.DMA((19,)),
            pltpu.SemaphoreType.DMA((16,)),
            pltpu.SemaphoreType.DMA((16,)),
        ],
        compiler_params=params(0),
    )(holder, tokens, small, wpk)


def add_rows(into, start, end, *others):
    @pl.loop(0, (end - start) // 16)
    def _(i):
        rows = pl.ds(pl.multiple_of(start + i * 16, 16), 16)
        total = into[rows].astype(jnp.float32)
        for other in others:
            total += other[pl.ds(pl.multiple_of(i * 16, 16), 16)].astype(jnp.float32)
        into[rows] = total.astype(into.dtype)


def scatter_kernel(
    att, w3, hw, out, hwx, parts, r, za, zb, fa0, fa1, ya, fb0, fb1, yb, send_sem, recv_sem, local_sem, hs, hr
):
    me = Place()
    sends = Sends(send_sem, recv_sem)
    up, down, over, twin = me.at(ry=1), me.at(ry=3), me.at(rz=1), me.twin()
    right, left, partner = me.at(rx=1), me.at(rx=3), me.across(me.c)
    greet([up, down, over, twin, right, left, partner])

    order = [(1, 2), (1, 0), (1, 1), (1, 3), (0, 2), (0, 1), (0, 3), (0, 0)]
    quarter = hw.shape[0] // 4
    half = quarter // 2

    def head_copy(k, start, size, device, src):
        rows = pl.ds(start, size)
        return pltpu.make_async_remote_copy(
            src_ref=src.at[rows],
            dst_ref=hwx.at[rows],
            send_sem=hs.at[k],
            recv_sem=hr.at[k],
            device_id=device,
            device_id_type=MESH,
        )

    head_out = head_copy(0, me.x * quarter, quarter, partner, hw)
    head_keep = pltpu.make_async_copy(hw, hwx, local_sem.at[0])
    head_right = head_copy(1, me.x * quarter, quarter, right, hwx)
    head_left = head_copy(2, me.x * quarter, quarter, left, hwx)
    head_right2 = head_copy(3, lax.rem(me.x + 3, 4) * quarter, half, right, hwx)
    head_left2 = head_copy(4, lax.rem(me.x + 1, 4) * quarter + half, half, left, hwx)

    @pl.when(me.n == 0)
    def _():
        head_out.start()
        head_keep.start()

    def project(slot, write):
        @pl.loop(0, out.shape[1] // 512)
        def _(i):
            part = pl.ds(pl.multiple_of(i * 512, 512), 512)
            write(
                part,
                lax.dot_general(
                    att[slot],
                    w3[part],
                    (((1,), (1,)), ((), ())),
                    preferred_element_type=jnp.float32,
                ),
            )

    def halve(rz, ry):
        j = rz * 4 + ry

        def write(part, value):
            parts[j, :, part] = value.astype(parts.dtype)

        project(me.other_slot(rz, ry), write)
        return sends.start(parts.at[j], r.at[j], twin)

    def merge(rz, ry):
        j = rz * 4 + ry

        def write(part, value):
            total = r[j, :, part].astype(jnp.float32) + value
            r[j, :, part] = total.astype(r.dtype)

        project(me.slot(rz, ry), write)

    a_got, b_got, y_got = {}, {}, {}
    halves = [halve(*order[0]), halve(*order[1])]
    for at, (rz, ry) in enumerate(order):
        if at + 2 < 8:
            halves.append(halve(*order[at + 2]))
        halves[at].wait_recv()
        block = r.at[rz * 4 + ry]
        merge(rz, ry)
        if rz == 1:
            a_got[ry] = sends.start(block.at[pl.ds(0, A_END)], za.at[ry], over)
        if ry == 2:
            b_got[rz, 0] = sends.start(block.at[pl.ds(A_END, B_MID - A_END)], fb0.at[rz], up)
            b_got[rz, 1] = sends.start(block.at[pl.ds(B_MID, 128 - B_MID)], fb1.at[rz], down)

    @pl.when(me.n == 1)
    def _():
        head_out.wait_recv()
        head_right.start()
        head_left.start()

    tail = pl.ds(A_END, 128 - A_END)
    for rz in (1, 0):
        b_got[rz, 0].wait_recv()
        add_rows(r.at[rz * 4 + 1], A_END, B_MID, fb0.at[rz])
        y_got[rz, 0] = sends.start(r.at[rz * 4 + 1, tail], yb.at[rz * 2], up)
        b_got[rz, 1].wait_recv()
        add_rows(r.at[rz * 4 + 3], B_MID, 128, fb1.at[rz])
        y_got[rz, 1] = sends.start(r.at[rz * 4 + 3, tail], yb.at[rz * 2 + 1], down)

    head = pl.ds(0, A_END)
    a_got[2].wait_recv()
    add_rows(r.at[2], 0, A_END, za.at[2])
    f_up = sends.start(r.at[2, pl.ds(0, A_MID)], fa0, up)
    f_down = sends.start(r.at[2, pl.ds(A_MID, A_END - A_MID)], fa1, down)

    y_got[1, 0].wait_recv()
    y_got[1, 1].wait_recv()
    add_rows(r.at[4], A_END, 128, yb.at[2], yb.at[3])
    z_got = sends.start(r.at[4, tail], zb, over)

    @pl.when(me.n == 1)
    def _():
        head_right.wait_recv()
        head_right2.start()
        head_left.wait_recv()
        head_left2.start()

    a_got[1].wait_recv()
    add_rows(r.at[1], 0, A_END, za.at[1])
    f_up.wait_recv()
    add_rows(r.at[1], 0, A_MID, fa0)
    g_up = sends.start(r.at[1, head], ya.at[0], up)
    a_got[3].wait_recv()
    add_rows(r.at[3], 0, A_END, za.at[3])
    f_down.wait_recv()
    add_rows(r.at[3], A_MID, A_END, fa1)
    g_down = sends.start(r.at[3, head], ya.at[1], down)

    def total(start, end, others):
        @pl.loop(0, (end - start) // 16)
        def _(i):
            here = pl.ds(pl.multiple_of(i * 16, 16), 16)
            rows = pl.ds(pl.multiple_of(start + i * 16, 16), 16)
            value = r[0, rows].astype(jnp.float32)
            for other in others:
                value += other[here].astype(jnp.float32)
            out[rows] = value

    y_got[0, 0].wait_recv()
    y_got[0, 1].wait_recv()
    z_got.wait_recv()
    total(A_END, 128, [yb.at[0], yb.at[1], zb])
    a_got[0].wait_recv()
    g_up.wait_recv()
    g_down.wait_recv()
    total(0, A_END, [za.at[0], ya.at[0], ya.at[1]])

    @pl.when(me.n == 1)
    def _():
        head_right2.wait_recv()
        head_left2.wait_recv()
        head_right.wait_send()
        head_left.wait_send()
        head_right2.wait_send()
        head_left2.wait_send()

    @pl.when(me.n == 0)
    def _():
        head_out.wait_send()
        head_keep.wait()

    sends.finish()


def scatter_parts(att, w3, hw):
    rows, width = att.shape[1], w3.shape[0]
    dtype = att.dtype
    return pl.pallas_call(
        scatter_kernel,
        name="scatter_parts",
        out_shape=(
            jax.ShapeDtypeStruct((rows, width), jnp.float32),
            jax.ShapeDtypeStruct(hw.shape, hw.dtype),
        ),
        in_specs=[VMEM] * 3,
        out_specs=(VMEM, ANY),
        scratch_shapes=[
            pltpu.VMEM((8, rows, width), dtype),
            pltpu.VMEM((8, rows, width), dtype),
            pltpu.VMEM((4, A_END, width), dtype),
            pltpu.VMEM((rows - A_END, width), dtype),
            pltpu.VMEM((A_MID, width), dtype),
            pltpu.VMEM((A_END - A_MID, width), dtype),
            pltpu.VMEM((2, A_END, width), dtype),
            pltpu.VMEM((2, B_MID - A_END, width), dtype),
            pltpu.VMEM((2, rows - B_MID, width), dtype),
            pltpu.VMEM((4, rows - A_END, width), dtype),
            pltpu.SemaphoreType.DMA((32,)),
            pltpu.SemaphoreType.DMA((32,)),
            pltpu.SemaphoreType.DMA((1,)),
            pltpu.SemaphoreType.DMA((5,)),
            pltpu.SemaphoreType.DMA((5,)),
        ],
        compiler_params=params(2),
    )(att, w3, hw)


def finish_kernel(
    summed,
    xown,
    gain,
    hw,
    tcol,
    loss,
    full,
    lg,
    cols,
    st,
    got,
    send_sem,
    recv_sem,
    local_sem,
    tell_send,
    tell_recv,
):
    me = Place()
    sends = Sends(send_sem, recv_sem)
    greet_plane(me)
    own = me.slot(0, 0)
    width = summed.shape[1]

    @pl.loop(0, 8)
    def _(i):
        rows = pl.ds(pl.multiple_of(i * 16, 16), 16)
        hidden = xown[rows].astype(jnp.float32) + summed[rows]
        mean = jnp.sum(hidden * hidden, axis=1, keepdims=True) * (1.0 / width)
        normed = hidden * lax.rsqrt(mean + 1e-05) * gain[...]
        full[own, rows] = normed.astype(full.dtype)

    blocks = BlockGather(me, full, sends)
    vocab = hw.shape[1]
    sender = me.c * 8 + me.fs

    def tell(b):
        return pltpu.make_async_remote_copy(
            src_ref=st.at[b],
            dst_ref=got.at[sender],
            send_sem=tell_send.at[b],
            recv_sem=tell_recv.at[sender],
            device_id=(me.x * 2 + me.g, lax.div(b, 2), lax.rem(b, 2)),
            device_id_type=MESH,
        )

    note = pltpu.make_async_copy(st.at[me.fm], got.at[sender], local_sem.at[0])

    def score(rz, ry):
        slots = (me.slot(rz, ry), me.other_slot(rz, ry))

        @pl.loop(0, vocab // 256)
        def _(i):
            part = pl.ds(pl.multiple_of(i * 256, 256), 256)
            pair = jnp.concatenate([full[slots[0]], full[slots[1]]], axis=0)
            lg[:, part] = jnp.dot(pair, hw[:, part], preferred_element_type=jnp.float32)

        for t, slot in enumerate(slots):

            @pl.loop(0, 8)
            def _(i):
                here = pl.ds(pl.multiple_of(t * 128 + i * 16, 16), 16)
                rows = pl.ds(pl.multiple_of(i * 16, 16), 16)
                logits = lg[here]
                top = jnp.max(logits, axis=1, keepdims=True)
                total = jnp.sum(jnp.exp(logits - top), axis=1, keepdims=True)
                ids = lax.broadcasted_iota(jnp.int32, logits.shape, 1) + own * vocab
                picked = jnp.sum(
                    jnp.where(ids == tcol[slot, rows], logits, 0.0), axis=1, keepdims=True
                )
                lane = lax.broadcasted_iota(jnp.int32, (16, 128), 1)
                cols[rows] = jnp.where(lane == 0, top, jnp.where(lane == 1, total, picked))

            st[slot] = cols[...].T[:8]

            @pl.when(jnp.logical_or(me.n == 1, slot != me.fm))
            def _():
                tell(slot).start()

            @pl.when(jnp.logical_and(me.n == 0, slot == me.fm))
            def _():
                note.start()

    blocks.first()
    blocks.twins[0].wait_recv()
    score(0, 0)
    blocks.second()
    blocks.third()
    blocks.twins[1].wait_recv()
    score(0, 1)
    blocks.fourth()
    blocks.twins[2].wait_recv()
    score(0, 3)
    blocks.twins[3].wait_recv()
    score(1, 0)
    blocks.wait("bf0", "bf1")
    blocks.share(0, 2)
    blocks.twins[4].wait_recv()
    score(1, 1)
    blocks.wait("az2", "bf2", "bf3")
    blocks.share(1, 2)
    blocks.twins[5].wait_recv()
    score(1, 3)
    blocks.twins[6].wait_recv()
    score(0, 2)
    blocks.twins[7].wait_recv()
    score(1, 2)

    @pl.loop(0, 16)
    def _(j):
        @pl.when(jnp.logical_or(me.n == 1, j != sender))
        def _():
            pltpu.make_async_remote_copy(
                src_ref=st.at[0],
                dst_ref=got.at[j],
                send_sem=tell_send.at[0],
                recv_sem=tell_recv.at[j],
                device_id=me.twin(),
                device_id_type=MESH,
            ).wait_recv()

    @pl.when(me.n == 0)
    def _():
        note.wait()

    top = got[0, 0:1]
    for j in range(1, 16):
        top = jnp.maximum(top, got[j, 0:1])
    total, picked = jnp.zeros_like(top), jnp.zeros_like(top)
    for j in range(16):
        total += got[j, 1:2] * jnp.exp(got[j, 0:1] - top)
        picked += got[j, 2:3]
    loss[...] = jnp.broadcast_to(top + jnp.log(total) - picked, loss.shape)

    @pl.loop(0, 16)
    def _(b):
        @pl.when(jnp.logical_or(me.n == 1, b != me.fm))
        def _():
            tell(b).wait_send()

    sends.finish()


def finish(summed, xown, gain, hw, tcol):
    rows, width = summed.shape
    return pl.pallas_call(
        finish_kernel,
        name="finish",
        out_shape=jax.ShapeDtypeStruct((8, rows), jnp.float32),
        in_specs=[VMEM] * 5,
        out_specs=VMEM,
        scratch_shapes=[
            pltpu.VMEM((16, rows, width), jnp.bfloat16),
            pltpu.VMEM((2 * rows, hw.shape[1]), jnp.float32),
            pltpu.VMEM((rows, 128), jnp.float32),
            pltpu.VMEM((16, 8, rows), jnp.float32),
            pltpu.VMEM((16, 8, rows), jnp.float32),
            pltpu.SemaphoreType.DMA((32,)),
            pltpu.SemaphoreType.DMA((32,)),
            pltpu.SemaphoreType.DMA((1,)),
            pltpu.SemaphoreType.DMA((16,)),
            pltpu.SemaphoreType.DMA((16,)),
        ],
        compiler_params=params(1),
    )(summed, xown, gain, hw, tcol)


def attend_kernel(x, w, seg_row, seg_col, out, q, k, vt):
    heads = out.shape[1] // HD
    seq = x.shape[0]
    size = 256

    @pl.loop(0, seq // size)
    def _(i):
        rows = pl.ds(pl.multiple_of(i * size, size), size)
        block = x[rows]
        q[rows] = jnp.dot(block, w[0], preferred_element_type=jnp.float32).astype(q.dtype)
        k[rows] = jnp.dot(block, w[1], preferred_element_type=jnp.float32).astype(k.dtype)
        v = jnp.dot(block, w[2], preferred_element_type=jnp.float32)
        vt[:, rows] = v.T.astype(vt.dtype)

    scale = math.log2(math.e) / math.sqrt(HD)

    @pl.loop(0, seq // size)
    def _(i):
        rows = pl.ds(pl.multiple_of(i * size, size), size)
        own = seg_row[0:1, rows]
        ahead = lax.broadcasted_iota(jnp.int32, (size, size), 0) - lax.broadcasted_iota(
            jnp.int32, (size, size), 1
        )

        def step(j, carry):
            cols = pl.ds(pl.multiple_of(j * size, size), size)
            allowed = (ahead <= (i - j) * size) & (seg_col[cols] == own)
            result = []
            for h in range(heads):
                part = pl.ds(h * HD, HD)
                top, total, acc = carry[h]
                score = lax.dot_general(
                    k[cols, part],
                    q[rows, part],
                    (((1,), (1,)), ((), ())),
                    preferred_element_type=jnp.float32,
                )
                score = jnp.where(allowed, score * scale, -1e30)
                new_top = jnp.maximum(top, jnp.max(score, axis=0, keepdims=True))
                prob = jnp.exp2(score - new_top)
                keep = jnp.exp2(top - new_top)
                total = total * keep + jnp.sum(prob, axis=0, keepdims=True)
                acc = acc * keep + jnp.dot(
                    vt[part, cols], prob.astype(vt.dtype), preferred_element_type=jnp.float32
                )
                result.append((new_top, total, acc))
            return tuple(result)

        start = (
            jnp.full((1, size), -1e30, jnp.float32),
            jnp.zeros((1, size), jnp.float32),
            jnp.zeros((HD, size), jnp.float32),
        )
        done = lax.fori_loop(0, i + 1, step, (start,) * heads)
        for h in range(heads):
            _, total, acc = done[h]
            out[rows, pl.ds(h * HD, HD)] = (acc / total).T.astype(out.dtype)


def attend(x, w, segments):
    seq = x.shape[0]
    cols = w.shape[2]
    return pl.pallas_call(
        attend_kernel,
        name="attend",
        out_shape=jax.ShapeDtypeStruct((seq, cols), x.dtype),
        in_specs=[VMEM] * 4,
        out_specs=VMEM,
        scratch_shapes=[
            pltpu.VMEM((seq, cols), x.dtype),
            pltpu.VMEM((seq, cols), x.dtype),
            pltpu.VMEM((cols, seq), x.dtype),
        ],
        compiler_params=pltpu.CompilerParams(vmem_limit_bytes=60 * 2**20),
        cost_estimate=pl.CostEstimate(
            flops=30 * 10**9, bytes_accessed=20 * 2**20, transcendentals=4 * 10**6
        ),
    )(x, w, segments[None, :], segments[:, None])


def inverse_of(table):
    total_count = table.shape[0]
    places = jnp.arange(total_count, dtype=jnp.int32)
    return jnp.sum(jnp.where(table[None, :] == places[:, None], places[None, :], 0), axis=1)


def pack_rows(stored, residues, fm_count):
    matrices, row_count, columns = stored.shape
    dp_count = residues.shape[0]
    split_rows = stored.reshape(
        matrices, row_count // dp_count, dp_count, fm_count, columns // fm_count
    )
    chosen = jnp.take(split_rows, residues, axis=2)
    return chosen.transpose(2, 3, 0, 1, 4).reshape(
        dp_count * fm_count, matrices, row_count // dp_count, columns // fm_count
    )


def unpack_rows(received, holder):
    ordered = jnp.take(received, holder, axis=0)
    devices, matrices, pair_rows, group_cols = ordered.shape
    return ordered.transpose(1, 0, 2, 3).reshape(matrices, devices * pair_rows, group_cols)


def everywhere(value):
    return lax.all_to_all(value, ("dp", "fsdp", "mp"), split_axis=0, concat_axis=0, tiled=True)


def body(
    tokens_in,
    segment_ids,
    target_ids,
    old_weights,
    old_first,
    old_second,
    old_block,
    new_residue,
    norm_gain,
    head_weight,
):
    me = Place()
    matrices, old_rows, columns = old_weights.shape
    groups = 16
    group_cols = columns // groups
    model_width = tokens_in.shape[1]

    tables = everywhere(jnp.broadcast_to(jnp.stack([old_block, new_residue], 1), (128, 2)))
    holder = inverse_of(tables[:, 0])
    residues = tables[::groups, 1]

    by_group = old_weights.reshape(matrices, old_rows, groups, group_cols).transpose(2, 0, 1, 3)
    by_group = by_group.reshape(groups, matrices * old_rows, group_cols)
    small = jnp.stack([segment_ids, target_ids] + [segment_ids] * 6)
    xfull, sfull, weights = gather_inputs(holder, tokens_in, small, by_group)

    whole_tokens = xfull.reshape(-1, model_width)
    segments = sfull[:, 0].reshape(-1)
    targets = sfull[:, 1][:, :, None]
    own = me.slot(0, 0)
    xown = lax.dynamic_index_in_dim(xfull, own, 0, keepdims=False)

    first, second, stored, weights = lax.optimization_barrier(
        (old_first, old_second, old_weights, weights)
    )
    moments = jnp.concatenate(
        [pack_rows(first, residues, groups), pack_rows(second, residues, groups)], axis=1
    )
    got_moments = everywhere(moments)
    got_weights = everywhere(pack_rows(stored, residues, groups))

    attended = attend(whole_tokens, weights[:3], segments)
    attended, got_moments, got_weights = lax.optimization_barrier(
        (attended, got_moments, got_weights)
    )
    summed, heads_used = scatter_parts(
        attended.reshape(16, -1, group_cols), weights[3], head_weight
    )
    loss = finish(summed, xown, norm_gain[None, :], heads_used, targets)[0]

    new_first = unpack_rows(got_moments[:, :matrices], holder)
    new_second = unpack_rows(got_moments[:, matrices:], holder)
    new_weights = unpack_rows(got_weights, holder)
    return (new_weights, new_first, new_second, loss)


def solution(mesh):
    placed = (
        P(("dp", "fsdp", "mp"), None),
        P(("dp", "fsdp", "mp")),
        P(("dp", "fsdp", "mp")),
        P(None, ("dp", "fsdp", "mp"), None),
        P(None, ("dp", "fsdp", "mp"), None),
        P(None, ("dp", "fsdp", "mp"), None),
        P(("dp", "fsdp", "mp")),
        P("dp"),
        P(),
        P(None, ("fsdp", "mp")),
    )
    return jax.shard_map(
        body,
        mesh=mesh,
        in_specs=placed,
        out_specs=(
            P(None, "dp", ("fsdp", "mp")),
            P(None, "dp", ("fsdp", "mp")),
            P(None, "dp", ("fsdp", "mp")),
            P(("dp", "fsdp", "mp")),
        ),
        check_vma=False,
    )
```

```python
import math

import jax
import jax.numpy as jnp
from jax import lax
from jax.experimental import pallas as pl
from jax.experimental.pallas import tpu as pltpu
from jax.sharding import PartitionSpec as P

HD = 128
MESH = pl.DeviceIdType.MESH
A_END, A_MID, B_MID = 48, 32, 80
VMEM = pl.BlockSpec(memory_space=pltpu.VMEM)
SMEM = pl.BlockSpec(memory_space=pltpu.SMEM)
ANY = pl.BlockSpec(memory_space=pl.ANY)


class Place:
    def __init__(self):
        self.dp = lax.axis_index("dp")
        self.fs = lax.axis_index("fsdp")
        self.g = lax.axis_index("mp")
        self.x, self.c = lax.div(self.dp, 2), lax.rem(self.dp, 2)
        self.zl, self.y = lax.div(self.fs, 4), lax.rem(self.fs, 4)
        self.fm = self.fs * 2 + self.g
        self.n = lax.rem(self.c + self.g, 2)

    def flip_z(self, rz):
        return 1 - self.zl if rz else self.zl

    def turn_y(self, ry):
        return lax.rem(self.y + ry, 4)

    def slot(self, rz, ry):
        z = self.flip_z(rz)
        return (z + self.n - 2 * z * self.n) * 8 + self.turn_y(ry) * 2 + self.c

    def other_slot(self, rz, ry):
        z, n = self.flip_z(rz), 1 - self.n
        return (z + n - 2 * z * n) * 8 + self.turn_y(ry) * 2 + 1 - self.c

    def at(self, rx=0, rz=0, ry=0):
        return (
            lax.rem(self.x + rx, 4) * 2 + self.c,
            self.flip_z(rz) * 4 + self.turn_y(ry),
            self.g,
        )

    def twin(self):
        return (self.x * 2 + 1 - self.c, self.fs, self.g)

    def across(self, core):
        return (self.x * 2 + core, (1 - self.zl) * 4 + self.y, 1 - self.g)


class Sends:
    def __init__(self, send_sem, recv_sem):
        self.send_sem, self.recv_sem, self.count, self.open = send_sem, recv_sem, 0, []

    def make(self, src, dst, device):
        k = self.count
        self.count += 1
        return pltpu.make_async_remote_copy(
            src_ref=src,
            dst_ref=dst,
            send_sem=self.send_sem.at[k],
            recv_sem=self.recv_sem.at[k],
            device_id=device,
            device_id_type=MESH,
        )

    def start(self, src, dst, device):
        copy = self.make(src, dst, device)
        copy.start()
        self.open.append(copy)
        return copy

    def finish(self):
        for copy in self.open:
            copy.wait_send()


def greet(devices):
    barrier = pltpu.get_barrier_semaphore()
    for device in devices:
        pl.semaphore_signal(barrier, inc=1, device_id=device, device_id_type=MESH)
    pl.semaphore_wait(barrier, len(devices))


def greet_plane(me, extra=()):
    barrier = pltpu.get_barrier_semaphore()

    @pl.loop(1, 32)
    def _(k):
        q = lax.rem(me.c * 16 + me.fm + k, 32)
        fm = lax.rem(q, 16)
        device = (me.x * 2 + lax.div(q, 16), lax.div(fm, 2), lax.rem(fm, 2))
        pl.semaphore_signal(barrier, inc=1, device_id=device, device_id_type=MESH)

    for device in extra:
        pl.semaphore_signal(barrier, inc=1, device_id=device, device_id_type=MESH)
    pl.semaphore_wait(barrier, 31 + len(extra))


class BlockGather:
    def __init__(self, me, full, sends):
        self.me, self.full, self.sends, self.got, self.twins = me, full, sends, {}, []

    def send(self, key, rz, ry, start, end, device):
        part = self.full.at[self.me.slot(rz, ry), pl.ds(start, end - start)]
        self.got[key] = self.sends.start(part, part, device)

    def wait(self, *keys):
        for key in keys:
            self.got[key].wait_recv()

    def share(self, rz, ry):
        block = self.full.at[self.me.slot(rz, ry)]
        self.twins.append(self.sends.start(block, block, self.me.twin()))

    def first(self):
        me = self.me
        self.up, self.down, self.over = me.at(ry=1), me.at(ry=3), me.at(rz=1)
        self.send("ay0", 0, 0, 0, A_END, self.up)
        self.send("ay1", 0, 0, 0, A_END, self.down)
        self.send("bz", 0, 0, A_END, 128, self.over)
        self.send("az0", 0, 0, 0, A_END, self.over)
        self.send("by0", 0, 0, A_END, 128, self.up)
        self.send("by1", 0, 0, A_END, 128, self.down)
        self.share(0, 0)

    def second(self):
        self.wait("ay0")
        self.send("af0", 0, 3, 0, A_MID, self.up)
        self.send("az3", 0, 3, 0, A_END, self.over)
        self.wait("ay1")
        self.send("af1", 0, 1, A_MID, A_END, self.down)
        self.send("az1", 0, 1, 0, A_END, self.over)
        self.wait("bz")
        self.send("by2", 1, 0, A_END, 128, self.up)
        self.send("by3", 1, 0, A_END, 128, self.down)

    def third(self):
        self.wait("af0", "af1")
        self.send("az2", 0, 2, 0, A_END, self.over)
        self.wait("by0")
        self.send("bf0", 0, 3, A_END, B_MID, self.up)
        self.wait("by1")
        self.send("bf1", 0, 1, B_MID, 128, self.down)
        self.share(0, 1)
        self.share(0, 3)
        self.wait("az0")
        self.share(1, 0)

    def fourth(self):
        self.wait("by2")
        self.send("bf2", 1, 3, A_END, B_MID, self.up)
        self.wait("by3")
        self.send("bf3", 1, 1, B_MID, 128, self.down)
        self.wait("az3", "az1")
        self.share(1, 1)
        self.share(1, 3)

    def last(self):
        self.wait("bf0", "bf1")
        self.share(0, 2)
        self.wait("az2", "bf2", "bf3")
        self.share(1, 2)
        for copy in self.twins:
            copy.wait_recv()


def gather_kernel(
    tok,
    small,
    mark,
    wpk,
    xfull,
    sfull,
    wlog,
    tables,
    wfull,
    wown,
    marks,
    holder,
    send_sem,
    recv_sem,
    local_sem,
    ex_send,
    ex_recv,
    small_send,
    small_recv,
    mark_send,
    mark_recv,
):
    me = Place()
    sends = Sends(send_sem, recv_sem)
    greet_plane(
        me,
        [
            (lax.rem(me.x + rx, 4) * 2 + core, me.fs, me.g)
            for rx in (1, 2, 3)
            for core in (0, 1)
        ],
    )

    keep = pltpu.make_async_copy(tok, xfull.at[me.fm], local_sem.at[0])
    swap = sends.make(tok, xfull.at[me.fm], me.across(1 - me.c))

    @pl.when(me.n == 0)
    def _():
        keep.start()

    @pl.when(me.n == 1)
    def _():
        swap.start()

    def exchange(k):
        t = lax.rem(me.fm + k, 16)
        return pltpu.make_async_remote_copy(
            src_ref=wpk.at[t],
            dst_ref=wown.at[me.fm],
            send_sem=ex_send.at[k],
            recv_sem=ex_recv.at[k],
            device_id=(me.dp, lax.div(t, 2), lax.rem(t, 2)),
            device_id_type=MESH,
        )

    place = me.dp * 16 + me.fm

    def mark_plane(k):
        t = lax.rem(me.fm + k, 16)
        return pltpu.make_async_remote_copy(
            src_ref=mark,
            dst_ref=marks.at[place],
            send_sem=mark_send.at[k],
            recv_sem=mark_recv.at[k],
            device_id=(me.dp, lax.div(t, 2), lax.rem(t, 2)),
            device_id_type=MESH,
        )

    def mark_rest(k):
        plane = marks.at[pl.ds(me.dp * 16, 16)]
        return pltpu.make_async_remote_copy(
            src_ref=plane,
            dst_ref=plane,
            send_sem=mark_send.at[16 + k],
            recv_sem=mark_recv.at[16 + k],
            device_id=(lax.rem(me.dp + k, 8), me.fs, me.g),
            device_id_type=MESH,
        )

    mark_own = pltpu.make_async_copy(mark, marks.at[place], local_sem.at[4])
    mark_own.start()

    @pl.loop(1, 16)
    def _(k):
        mark_plane(k).start()

    @pl.loop(1, 16)
    def _(k):
        exchange(k).start()

    own = pltpu.make_async_copy(wpk.at[me.fm], wown.at[me.fm], local_sem.at[1])
    own.start()

    def tell(k):
        q = lax.rem(me.c * 8 + me.fs + k, 16)
        return pltpu.make_async_remote_copy(
            src_ref=small,
            dst_ref=sfull.at[me.fm],
            send_sem=small_send.at[k],
            recv_sem=small_recv.at[me.fm],
            device_id=(me.x * 2 + lax.div(q, 8), lax.rem(q, 8), me.c),
            device_id_type=MESH,
        )

    note = pltpu.make_async_copy(small, sfull.at[me.fm], local_sem.at[2])

    @pl.when(me.n == 1)
    def _():
        tell(0).start()

    @pl.when(me.n == 0)
    def _():
        note.start()

    @pl.loop(1, 16)
    def _(k):
        tell(k).start()

    @pl.when(me.n == 0)
    def _():
        keep.wait()

    @pl.when(me.n == 1)
    def _():
        swap.wait_recv()

    blocks = BlockGather(me, xfull, sends)
    blocks.first()

    mark_own.wait()

    @pl.loop(1, 16)
    def _(k):
        mark_plane(k).wait_recv()

    @pl.loop(1, 8)
    def _(k):
        mark_rest(k).start()

    own.wait()

    @pl.loop(1, 16)
    def _(k):
        exchange(k).wait_recv()

    far = pltpu.make_async_remote_copy(
        src_ref=wown,
        dst_ref=wfull.at[pl.ds(me.dp * 16, 16)],
        send_sem=ex_send.at[16],
        recv_sem=ex_recv.at[16 + me.c],
        device_id=me.across(me.g),
        device_id_type=MESH,
    )
    far.start()
    near = pltpu.make_async_remote_copy(
        src_ref=wown,
        dst_ref=wfull.at[pl.ds(me.dp * 16, 16)],
        send_sem=ex_send.at[17],
        recv_sem=ex_recv.at[18],
        device_id=me.twin(),
        device_id_type=MESH,
    )
    stay = pltpu.make_async_copy(wown, wfull.at[pl.ds(me.dp * 16, 16)], local_sem.at[3])

    @pl.when(me.n == 1)
    def _():
        near.start()

    @pl.when(me.n == 0)
    def _():
        stay.start()

    blocks.second()

    def from_core(core):
        return pltpu.make_async_remote_copy(
            src_ref=wown,
            dst_ref=wfull.at[pl.ds(me.dp * 16, 16)],
            send_sem=ex_send.at[16],
            recv_sem=ex_recv.at[16 + core],
            device_id=me.across(me.g),
            device_id_type=MESH,
        )

    @pl.when(me.n == 1)
    def _():
        from_core(0).wait_recv()
        from_core(1).wait_recv()

    @pl.when(me.n == 0)
    def _():
        near.wait_recv()
        stay.wait()

    right, left = me.at(rx=1), me.at(rx=3)
    pair = wfull.at[pl.ds(me.x * 32, 32)]
    to_right = sends.start(pair, pair, right)
    to_left = sends.start(pair, pair, left)

    @pl.loop(1, 8)
    def _(k):
        mark_rest(k).wait_recv()

    lane = lax.broadcasted_iota(jnp.int32, (8, 128), 1)
    line = lax.broadcasted_iota(jnp.int32, (8, 128), 0)
    found = lax.fori_loop(
        0,
        128,
        lambda p, total: total + jnp.where(marks[p] == lane, p, 0),
        jnp.zeros((8, 128), jnp.int32),
    )
    residues = jnp.zeros((8, 128), jnp.int32)
    for i in range(8):
        residues += jnp.where(lane == i, marks[i * 16], 0)
    tables[...] = jnp.where(line == 0, jnp.minimum(found, 127), residues)
    tell_scalar = pltpu.make_async_copy(tables, holder, local_sem.at[5])
    tell_scalar.start()
    blocks.third()
    blocks.fourth()
    to_right.wait_recv()
    first = wfull.at[pl.ds(lax.rem(me.x + 3, 4) * 32, 16)]
    on_right = sends.start(first, first, right)
    to_left.wait_recv()
    second = wfull.at[pl.ds(lax.rem(me.x + 1, 4) * 32 + 16, 16)]
    on_left = sends.start(second, second, left)
    blocks.last()
    on_right.wait_recv()
    on_left.wait_recv()

    rows = wpk.shape[1] // 4
    tell_scalar.wait()

    @pl.loop(0, 128)
    def _(b):
        where = holder[0, b]
        for m in range(4):
            wlog[m, pl.ds(pl.multiple_of(b * rows, 8), rows)] = wfull[
                where, pl.ds(m * rows, rows)
            ]

    @pl.loop(0, 16)
    def _(j):
        @pl.when(jnp.logical_or(me.n == 1, j != me.fm))
        def _():
            pltpu.make_async_remote_copy(
                src_ref=small,
                dst_ref=sfull.at[j],
                send_sem=small_send.at[0],
                recv_sem=small_recv.at[j],
                device_id=me.twin(),
                device_id_type=MESH,
            ).wait_recv()

    @pl.loop(1, 16)
    def _(k):
        exchange(k).wait_send()
        tell(k).wait_send()
        mark_plane(k).wait_send()

    @pl.loop(1, 8)
    def _(k):
        mark_rest(k).wait_send()

    far.wait_send()

    @pl.when(me.n == 1)
    def _():
        tell(0).wait_send()
        near.wait_send()
        swap.wait_send()

    @pl.when(me.n == 0)
    def _():
        note.wait()

    sends.finish()


def params(collective_id):
    return pltpu.CompilerParams(
        collective_id=collective_id, has_side_effects=True, vmem_limit_bytes=60 * 2**20
    )


def gather_inputs(tokens, small, mark, wpk):
    rows, width = tokens.shape
    old_rows = wpk.shape[1] // 4
    return pl.pallas_call(
        gather_kernel,
        name="gather_inputs",
        out_shape=(
            jax.ShapeDtypeStruct((16, rows, width), tokens.dtype),
            jax.ShapeDtypeStruct((16, *small.shape), small.dtype),
            jax.ShapeDtypeStruct((4, 128 * old_rows, wpk.shape[2]), wpk.dtype),
            jax.ShapeDtypeStruct((8, 128), jnp.int32),
        ),
        in_specs=[VMEM] * 4,
        out_specs=(ANY, VMEM, VMEM, VMEM),
        scratch_shapes=[
            pltpu.VMEM((128, *wpk.shape[1:]), wpk.dtype),
            pltpu.VMEM(wpk.shape, wpk.dtype),
            pltpu.VMEM((128, 8, 128), jnp.int32),
            pltpu.SMEM((8, 128), jnp.int32),
            pltpu.SemaphoreType.DMA((40,)),
            pltpu.SemaphoreType.DMA((40,)),
            pltpu.SemaphoreType.DMA((6,)),
            pltpu.SemaphoreType.DMA((18,)),
            pltpu.SemaphoreType.DMA((19,)),
            pltpu.SemaphoreType.DMA((16,)),
            pltpu.SemaphoreType.DMA((16,)),
            pltpu.SemaphoreType.DMA((24,)),
            pltpu.SemaphoreType.DMA((24,)),
        ],
        compiler_params=params(0),
    )(tokens, small, mark, wpk)


def add_rows(into, start, end, *others):
    @pl.loop(0, (end - start) // 16)
    def _(i):
        rows = pl.ds(pl.multiple_of(start + i * 16, 16), 16)
        total = into[rows].astype(jnp.float32)
        for other in others:
            total += other[pl.ds(pl.multiple_of(i * 16, 16), 16)].astype(jnp.float32)
        into[rows] = total.astype(into.dtype)


def scatter_kernel(
    tables, att, w, hw, out, hwx, nw, tw, parts, r, za, zb, fa0, fa1, ya, fb0, fb1, yb, send_sem, recv_sem, local_sem, hs, hr
):
    me = Place()
    sends = Sends(send_sem, recv_sem)
    up, down, over, twin = me.at(ry=1), me.at(ry=3), me.at(rz=1), me.twin()
    right, left, partner = me.at(rx=1), me.at(rx=3), me.across(me.c)
    greet([up, down, over, twin, right, left, partner])

    order = [(1, 2), (1, 0), (1, 1), (1, 3), (0, 2), (0, 1), (0, 3), (0, 0)]
    quarter = hw.shape[0] // 4
    half = quarter // 2

    def head_copy(k, start, size, device, src):
        rows = pl.ds(start, size)
        return pltpu.make_async_remote_copy(
            src_ref=src.at[rows],
            dst_ref=hwx.at[rows],
            send_sem=hs.at[k],
            recv_sem=hr.at[k],
            device_id=device,
            device_id_type=MESH,
        )

    head_out = head_copy(0, me.x * quarter, quarter, partner, hw)
    head_keep = pltpu.make_async_copy(hw, hwx, local_sem.at[0])
    head_right = head_copy(1, me.x * quarter, quarter, right, hwx)
    head_left = head_copy(2, me.x * quarter, quarter, left, hwx)
    head_right2 = head_copy(3, lax.rem(me.x + 3, 4) * quarter, half, right, hwx)
    head_left2 = head_copy(4, lax.rem(me.x + 1, 4) * quarter + half, half, left, hwx)

    @pl.when(me.n == 0)
    def _():
        head_out.start()
        head_keep.start()

    def project(slot, write):
        @pl.loop(0, out.shape[1] // 512)
        def _(i):
            part = pl.ds(pl.multiple_of(i * 512, 512), 512)
            write(
                part,
                lax.dot_general(
                    att[slot],
                    w[3, part],
                    (((1,), (1,)), ((), ())),
                    preferred_element_type=jnp.float32,
                ),
            )

    def halve(rz, ry):
        j = rz * 4 + ry

        def write(part, value):
            parts[j, :, part] = value.astype(parts.dtype)

        project(me.other_slot(rz, ry), write)
        return sends.start(parts.at[j], r.at[j], twin)

    def merge(rz, ry):
        j = rz * 4 + ry

        def write(part, value):
            total = r[j, :, part].astype(jnp.float32) + value
            r[j, :, part] = total.astype(r.dtype)

        project(me.slot(rz, ry), write)

    a_got, b_got, y_got = {}, {}, {}
    halves = [halve(*order[0]), halve(*order[1])]
    for at, (rz, ry) in enumerate(order):
        if at + 2 < 8:
            halves.append(halve(*order[at + 2]))
        halves[at].wait_recv()
        block = r.at[rz * 4 + ry]
        merge(rz, ry)
        if rz == 1:
            a_got[ry] = sends.start(block.at[pl.ds(0, A_END)], za.at[ry], over)
        if ry == 2:
            b_got[rz, 0] = sends.start(block.at[pl.ds(A_END, B_MID - A_END)], fb0.at[rz], up)
            b_got[rz, 1] = sends.start(block.at[pl.ds(B_MID, 128 - B_MID)], fb1.at[rz], down)

    @pl.when(me.n == 1)
    def _():
        head_out.wait_recv()
        head_right.start()
        head_left.start()

    give = sends.make(tw, nw, twin)

    @pl.when(me.n == 0)
    def _():
        lane = lax.broadcasted_iota(jnp.int32, (64, 256), 1)
        line = lax.broadcasted_iota(jnp.int32, (64, 256), 0)
        mine, other = tables[1, me.dp], tables[1, me.x * 2 + 1 - me.c]
        wanted = jnp.where(line < 32, line * 8 + mine, (line - 32) * 8 + other)
        pick = jnp.where(lane == wanted, 1.0, 0.0).astype(w.dtype)
        for m in range(4):

            @pl.loop(0, w.shape[1] // 256)
            def _(t):
                rows = pl.ds(pl.multiple_of(t * 256, 256), 256)
                chosen = jnp.dot(pick, w[m, rows], preferred_element_type=jnp.float32)
                chosen = chosen.astype(nw.dtype)
                to = pl.ds(pl.multiple_of(t * 32, 32), 32)
                nw[m, to] = chosen[:32]
                tw[m, to] = chosen[32:]

        give.start()

    tail = pl.ds(A_END, 128 - A_END)
    for rz in (1, 0):
        b_got[rz, 0].wait_recv()
        add_rows(r.at[rz * 4 + 1], A_END, B_MID, fb0.at[rz])
        y_got[rz, 0] = sends.start(r.at[rz * 4 + 1, tail], yb.at[rz * 2], up)
        b_got[rz, 1].wait_recv()
        add_rows(r.at[rz * 4 + 3], B_MID, 128, fb1.at[rz])
        y_got[rz, 1] = sends.start(r.at[rz * 4 + 3, tail], yb.at[rz * 2 + 1], down)

    head = pl.ds(0, A_END)
    a_got[2].wait_recv()
    add_rows(r.at[2], 0, A_END, za.at[2])
    f_up = sends.start(r.at[2, pl.ds(0, A_MID)], fa0, up)
    f_down = sends.start(r.at[2, pl.ds(A_MID, A_END - A_MID)], fa1, down)

    y_got[1, 0].wait_recv()
    y_got[1, 1].wait_recv()
    add_rows(r.at[4], A_END, 128, yb.at[2], yb.at[3])
    z_got = sends.start(r.at[4, tail], zb, over)

    @pl.when(me.n == 1)
    def _():
        head_right.wait_recv()
        head_right2.start()
        head_left.wait_recv()
        head_left2.start()

    a_got[1].wait_recv()
    add_rows(r.at[1], 0, A_END, za.at[1])
    f_up.wait_recv()
    add_rows(r.at[1], 0, A_MID, fa0)
    g_up = sends.start(r.at[1, head], ya.at[0], up)
    a_got[3].wait_recv()
    add_rows(r.at[3], 0, A_END, za.at[3])
    f_down.wait_recv()
    add_rows(r.at[3], A_MID, A_END, fa1)
    g_down = sends.start(r.at[3, head], ya.at[1], down)

    def total(start, end, others):
        @pl.loop(0, (end - start) // 16)
        def _(i):
            here = pl.ds(pl.multiple_of(i * 16, 16), 16)
            rows = pl.ds(pl.multiple_of(start + i * 16, 16), 16)
            value = r[0, rows].astype(jnp.float32)
            for other in others:
                value += other[here].astype(jnp.float32)
            out[rows] = value

    y_got[0, 0].wait_recv()
    y_got[0, 1].wait_recv()
    z_got.wait_recv()
    total(A_END, 128, [yb.at[0], yb.at[1], zb])
    a_got[0].wait_recv()
    g_up.wait_recv()
    g_down.wait_recv()
    total(0, A_END, [za.at[0], ya.at[0], ya.at[1]])

    @pl.when(me.n == 1)
    def _():
        give.wait_recv()
        head_right2.wait_recv()
        head_left2.wait_recv()
        head_right.wait_send()
        head_left.wait_send()
        head_right2.wait_send()
        head_left2.wait_send()

    @pl.when(me.n == 0)
    def _():
        give.wait_send()
        head_out.wait_send()
        head_keep.wait()

    sends.finish()


def scatter_parts(tables, att, w, hw):
    rows, width = att.shape[1], w.shape[1]
    kept = (w.shape[0], width // 8, w.shape[2])
    dtype = att.dtype
    return pl.pallas_call(
        scatter_kernel,
        name="scatter_parts",
        out_shape=(
            jax.ShapeDtypeStruct((rows, width), jnp.float32),
            jax.ShapeDtypeStruct(hw.shape, hw.dtype),
            jax.ShapeDtypeStruct(kept, w.dtype),
        ),
        in_specs=[SMEM] + [VMEM] * 3,
        out_specs=(VMEM, ANY, VMEM),
        scratch_shapes=[
            pltpu.VMEM(kept, w.dtype),
            pltpu.VMEM((8, rows, width), dtype),
            pltpu.VMEM((8, rows, width), dtype),
            pltpu.VMEM((4, A_END, width), dtype),
            pltpu.VMEM((rows - A_END, width), dtype),
            pltpu.VMEM((A_MID, width), dtype),
            pltpu.VMEM((A_END - A_MID, width), dtype),
            pltpu.VMEM((2, A_END, width), dtype),
            pltpu.VMEM((2, B_MID - A_END, width), dtype),
            pltpu.VMEM((2, rows - B_MID, width), dtype),
            pltpu.VMEM((4, rows - A_END, width), dtype),
            pltpu.SemaphoreType.DMA((32,)),
            pltpu.SemaphoreType.DMA((32,)),
            pltpu.SemaphoreType.DMA((1,)),
            pltpu.SemaphoreType.DMA((5,)),
            pltpu.SemaphoreType.DMA((5,)),
        ],
        compiler_params=params(2),
    )(tables, att, w, hw)


def finish_kernel(
    summed,
    xown,
    gain,
    hw,
    tcol,
    loss,
    full,
    lg,
    cols,
    st,
    got,
    send_sem,
    recv_sem,
    local_sem,
    tell_send,
    tell_recv,
):
    me = Place()
    sends = Sends(send_sem, recv_sem)
    greet_plane(me)
    own = me.slot(0, 0)
    width = summed.shape[1]

    @pl.loop(0, 8)
    def _(i):
        rows = pl.ds(pl.multiple_of(i * 16, 16), 16)
        hidden = xown[rows].astype(jnp.float32) + summed[rows]
        mean = jnp.sum(hidden * hidden, axis=1, keepdims=True) * (1.0 / width)
        normed = hidden * lax.rsqrt(mean + 1e-05) * gain[...]
        full[own, rows] = normed.astype(full.dtype)

    blocks = BlockGather(me, full, sends)
    vocab = hw.shape[1]
    sender = me.c * 8 + me.fs

    def tell(b):
        return pltpu.make_async_remote_copy(
            src_ref=st.at[b],
            dst_ref=got.at[sender],
            send_sem=tell_send.at[b],
            recv_sem=tell_recv.at[sender],
            device_id=(me.x * 2 + me.g, lax.div(b, 2), lax.rem(b, 2)),
            device_id_type=MESH,
        )

    note = pltpu.make_async_copy(st.at[me.fm], got.at[sender], local_sem.at[0])

    def score(*pairs):
        slots = [slot(rz, ry) for rz, ry in pairs for slot in (me.slot, me.other_slot)]
        rows = pl.ds(0, 128 * len(slots))

        @pl.loop(0, vocab // 256)
        def _(i):
            part = pl.ds(pl.multiple_of(i * 256, 256), 256)
            block = jnp.concatenate([full[slot] for slot in slots], axis=0)
            lg[rows, part] = jnp.dot(block, hw[:, part], preferred_element_type=jnp.float32)

        for t, slot in enumerate(slots):

            @pl.loop(0, 4)
            def _(i):
                here = pl.ds(pl.multiple_of(t * 128 + i * 32, 32), 32)
                to = pl.ds(pl.multiple_of(i * 32, 32), 32)
                parts = [lg[here, pl.ds(j * 128, 128)] for j in range(vocab // 128)]
                top = parts[0]
                for part in parts[1:]:
                    top = jnp.maximum(top, part)
                wanted = tcol[slot, to] - own * vocab
                ids = lax.broadcasted_iota(jnp.int32, top.shape, 1)
                total, picked = jnp.zeros_like(top), jnp.zeros_like(top)
                for j, part in enumerate(parts):
                    total += jnp.exp(part - top)
                    picked += jnp.where(ids + j * 128 == wanted, part, 0.0)
                cols[0, to], cols[1, to], cols[2, to] = top, total, picked

            tops = cols[0].T
            top = jnp.max(tops, axis=0, keepdims=True)
            total = jnp.sum(cols[1].T * jnp.exp(tops - top), axis=0, keepdims=True)
            picked = jnp.sum(cols[2].T, axis=0, keepdims=True)
            st[slot] = jnp.concatenate([top, total, picked, jnp.zeros((5, 128))], axis=0)

            @pl.when(jnp.logical_or(me.n == 1, slot != me.fm))
            def _():
                tell(slot).start()

            @pl.when(jnp.logical_and(me.n == 0, slot == me.fm))
            def _():
                note.start()

    def twins(*which):
        for k in which:
            blocks.twins[k].wait_recv()

    blocks.first()
    twins(0)
    score((0, 0))
    blocks.second()
    blocks.third()
    twins(1, 2)
    score((0, 1), (0, 3))
    blocks.fourth()
    blocks.wait("bf0", "bf1")
    blocks.share(0, 2)
    twins(3, 4)
    score((1, 0), (1, 1))
    blocks.wait("az2", "bf2", "bf3")
    blocks.share(1, 2)
    twins(5, 6)
    score((1, 3), (0, 2))
    twins(7)
    score((1, 2))

    @pl.loop(0, 16)
    def _(j):
        @pl.when(jnp.logical_or(me.n == 1, j != sender))
        def _():
            pltpu.make_async_remote_copy(
                src_ref=st.at[0],
                dst_ref=got.at[j],
                send_sem=tell_send.at[0],
                recv_sem=tell_recv.at[j],
                device_id=me.twin(),
                device_id_type=MESH,
            ).wait_recv()

    @pl.when(me.n == 0)
    def _():
        note.wait()

    top = got[0, 0:1]
    for j in range(1, 16):
        top = jnp.maximum(top, got[j, 0:1])
    total, picked = jnp.zeros_like(top), jnp.zeros_like(top)
    for j in range(16):
        total += got[j, 1:2] * jnp.exp(got[j, 0:1] - top)
        picked += got[j, 2:3]
    loss[...] = jnp.broadcast_to(top + jnp.log(total) - picked, loss.shape)

    @pl.loop(0, 16)
    def _(b):
        @pl.when(jnp.logical_or(me.n == 1, b != me.fm))
        def _():
            tell(b).wait_send()

    sends.finish()


def finish(summed, xown, gain, hw, tcol):
    rows, width = summed.shape
    return pl.pallas_call(
        finish_kernel,
        name="finish",
        out_shape=jax.ShapeDtypeStruct((8, rows), jnp.float32),
        in_specs=[VMEM] * 5,
        out_specs=VMEM,
        scratch_shapes=[
            pltpu.VMEM((16, rows, width), jnp.bfloat16),
            pltpu.VMEM((4 * rows, hw.shape[1]), jnp.float32),
            pltpu.VMEM((3, rows, 128), jnp.float32),
            pltpu.VMEM((16, 8, rows), jnp.float32),
            pltpu.VMEM((16, 8, rows), jnp.float32),
            pltpu.SemaphoreType.DMA((32,)),
            pltpu.SemaphoreType.DMA((32,)),
            pltpu.SemaphoreType.DMA((1,)),
            pltpu.SemaphoreType.DMA((16,)),
            pltpu.SemaphoreType.DMA((16,)),
        ],
        compiler_params=params(1),
    )(summed, xown, gain, hw, tcol)


def attend_kernel(
    tables,
    x,
    w,
    seg_row,
    seg_col,
    first,
    second,
    out,
    new_first,
    new_second,
    q,
    k,
    vt,
    packed,
    got,
    send_sem,
    recv_sem,
    local_sem,
):
    heads = out.shape[1] // HD
    seq = x.shape[0]
    size = 256
    me = Place()
    place = me.dp * 16 + me.fm
    barrier = pltpu.get_barrier_semaphore()

    @pl.loop(1, 128)
    def _(t):
        p = lax.rem(place + t, 128)
        fm = lax.rem(p, 16)
        device = (lax.div(p, 16), lax.div(fm, 2), lax.rem(fm, 2))
        pl.semaphore_signal(barrier, inc=1, device_id=device, device_id_type=MESH)

    @pl.loop(0, 8)
    def _(i):
        residue = tables[1, i]
        for s, source in enumerate((first, second)):
            for m in range(4):
                for j in range(3):
                    packed[i, pl.ds(s * 12 + m * 3 + j, 1)] = source[m, pl.ds(j * 8 + residue, 1)]

    pl.semaphore_wait(barrier, 127)

    def spread(t):
        p = lax.rem(place + t, 128)
        dp, fm = lax.div(p, 16), lax.rem(p, 16)
        return pltpu.make_async_remote_copy(
            src_ref=packed.at[dp, :, pl.ds(pl.multiple_of(fm * 256, 256), 256)],
            dst_ref=got.at[place],
            send_sem=send_sem.at[t],
            recv_sem=recv_sem.at[t],
            device_id=(dp, lax.div(fm, 2), lax.rem(fm, 2)),
            device_id_type=MESH,
        )

    @pl.loop(1, 128)
    def _(t):
        spread(t).start()

    keep = pltpu.make_async_copy(
        packed.at[me.dp, :, pl.ds(pl.multiple_of(me.fm * 256, 256), 256)],
        got.at[place],
        local_sem.at[0],
    )
    keep.start()

    @pl.loop(0, seq // size)
    def _(i):
        rows = pl.ds(pl.multiple_of(i * size, size), size)
        block = x[rows]
        q[rows] = jnp.dot(block, w[0], preferred_element_type=jnp.float32).astype(q.dtype)
        k[rows] = jnp.dot(block, w[1], preferred_element_type=jnp.float32).astype(k.dtype)
        v = jnp.dot(block, w[2], preferred_element_type=jnp.float32)
        vt[:, rows] = v.T.astype(vt.dtype)

    scale = math.log2(math.e) / math.sqrt(HD)

    @pl.loop(0, seq // size)
    def _(i):
        rows = pl.ds(pl.multiple_of(i * size, size), size)
        own = seg_row[0:1, rows]
        ahead = lax.broadcasted_iota(jnp.int32, (size, size), 0) - lax.broadcasted_iota(
            jnp.int32, (size, size), 1
        )

        def step(j, carry):
            cols = pl.ds(pl.multiple_of(j * size, size), size)
            allowed = (ahead <= (i - j) * size) & (seg_col[cols] == own)
            result = []
            for h in range(heads):
                part = pl.ds(h * HD, HD)
                top, total, acc = carry[h]
                score = lax.dot_general(
                    k[cols, part],
                    q[rows, part],
                    (((1,), (1,)), ((), ())),
                    preferred_element_type=jnp.float32,
                )
                score = jnp.where(allowed, score * scale, -1e30)
                new_top = jnp.maximum(top, jnp.max(score, axis=0, keepdims=True))
                prob = jnp.exp2(score - new_top)
                keep = jnp.exp2(top - new_top)
                total = total * keep + jnp.sum(prob, axis=0, keepdims=True)
                acc = acc * keep + jnp.dot(
                    vt[part, cols], prob.astype(vt.dtype), preferred_element_type=jnp.float32
                )
                result.append((new_top, total, acc))
            return tuple(result)

        start = (
            jnp.full((1, size), -1e30, jnp.float32),
            jnp.zeros((1, size), jnp.float32),
            jnp.zeros((HD, size), jnp.float32),
        )
        done = lax.fori_loop(0, i + 1, step, (start,) * heads)
        for h in range(heads):
            _, total, acc = done[h]
            out[rows, pl.ds(h * HD, HD)] = (acc / total).T.astype(out.dtype)

    keep.wait()

    @pl.loop(1, 128)
    def _(t):
        spread(t).wait_recv()

    @pl.loop(0, 16)
    def _(t):
        holders = [tables[0, t * 8 + u] for u in range(8)]
        rows = pl.ds(pl.multiple_of(t * 24, 8), 24)
        for s, target in enumerate((new_first, new_second)):
            for m in range(4):
                target[m, rows] = jnp.concatenate(
                    [got[p, pl.ds(s * 12 + m * 3, 3)] for p in holders], axis=0
                )

    @pl.loop(1, 128)
    def _(t):
        spread(t).wait_send()


def attend(tables, x, w, segments, first, second):
    seq = x.shape[0]
    cols = w.shape[2]
    moment = jax.ShapeDtypeStruct((4, w.shape[1] // 8, cols), first.dtype)
    return pl.pallas_call(
        attend_kernel,
        name="attend",
        out_shape=(jax.ShapeDtypeStruct((seq, cols), x.dtype), moment, moment),
        in_specs=[SMEM] + [VMEM] * 6,
        out_specs=(VMEM,) * 3,
        scratch_shapes=[
            pltpu.VMEM((seq, cols), x.dtype),
            pltpu.VMEM((seq, cols), x.dtype),
            pltpu.VMEM((cols, seq), x.dtype),
            pltpu.VMEM((8, 24, 16 * cols), first.dtype),
            pltpu.VMEM((128, 24, cols), first.dtype),
            pltpu.SemaphoreType.DMA((128,)),
            pltpu.SemaphoreType.DMA((128,)),
            pltpu.SemaphoreType.DMA((1,)),
        ],
        compiler_params=params(3),
    )(tables, x, w, segments[None, :], segments[:, None], first, second)


def body(
    tokens_in,
    segment_ids,
    target_ids,
    old_weights,
    old_first,
    old_second,
    old_block,
    new_residue,
    norm_gain,
    head_weight,
):
    me = Place()
    matrices, old_rows, columns = old_weights.shape
    groups = 16
    group_cols = columns // groups
    model_width = tokens_in.shape[1]

    by_group = old_weights.reshape(matrices, old_rows, groups, group_cols).transpose(2, 0, 1, 3)
    by_group = by_group.reshape(groups, matrices * old_rows, group_cols)
    small = jnp.stack([segment_ids, target_ids] + [segment_ids] * 6)
    mark = jnp.where(jnp.arange(8)[:, None] == 0, old_block[0], new_residue[0])
    mark = jnp.broadcast_to(mark, (8, 128)).astype(jnp.int32)
    xfull, sfull, weights, tables = gather_inputs(tokens_in, small, mark, by_group)

    segments = sfull[:, 0].reshape(-1)
    targets = sfull[:, 1][:, :, None]
    own = me.slot(0, 0)
    xown = lax.dynamic_index_in_dim(xfull, own, 0, keepdims=False)

    attended, new_first, new_second = attend(
        tables, xfull.reshape(-1, model_width), weights, segments, old_first, old_second
    )
    summed, heads_used, new_weights = scatter_parts(
        tables, attended.reshape(16, -1, group_cols), weights, head_weight
    )
    loss = finish(summed, xown, norm_gain[None, :], heads_used, targets)[0]
    return (new_weights, new_first, new_second, loss)


def solution(mesh):
    placed = (
        P(("dp", "fsdp", "mp"), None),
        P(("dp", "fsdp", "mp")),
        P(("dp", "fsdp", "mp")),
        P(None, ("dp", "fsdp", "mp"), None),
        P(None, ("dp", "fsdp", "mp"), None),
        P(None, ("dp", "fsdp", "mp"), None),
        P(("dp", "fsdp", "mp")),
        P("dp"),
        P(),
        P(None, ("fsdp", "mp")),
    )
    return jax.shard_map(
        body,
        mesh=mesh,
        in_specs=placed,
        out_specs=(
            P(None, "dp", ("fsdp", "mp")),
            P(None, "dp", ("fsdp", "mp")),
            P(None, "dp", ("fsdp", "mp")),
            P(("dp", "fsdp", "mp")),
        ),
        check_vma=False,
    )
```

```python
import math

import jax
import jax.numpy as jnp
from jax import lax
from jax.experimental import pallas as pl
from jax.experimental.pallas import tpu as pltpu
from jax.sharding import PartitionSpec as P

HD = 128
MESH = pl.DeviceIdType.MESH
A_END, A_MID, B_MID = 48, 32, 80
VMEM = pl.BlockSpec(memory_space=pltpu.VMEM)
SMEM = pl.BlockSpec(memory_space=pltpu.SMEM)
ANY = pl.BlockSpec(memory_space=pl.ANY)


class Place:
    def __init__(self):
        self.dp = lax.axis_index("dp")
        self.fs = lax.axis_index("fsdp")
        self.g = lax.axis_index("mp")
        self.x, self.c = lax.div(self.dp, 2), lax.rem(self.dp, 2)
        self.zl, self.y = lax.div(self.fs, 4), lax.rem(self.fs, 4)
        self.fm = self.fs * 2 + self.g
        self.n = lax.rem(self.c + self.g, 2)

    def flip_z(self, rz):
        return 1 - self.zl if rz else self.zl

    def turn_y(self, ry):
        return lax.rem(self.y + ry, 4)

    def slot(self, rz, ry):
        z = self.flip_z(rz)
        return (z + self.n - 2 * z * self.n) * 8 + self.turn_y(ry) * 2 + self.c

    def other_slot(self, rz, ry):
        z, n = self.flip_z(rz), 1 - self.n
        return (z + n - 2 * z * n) * 8 + self.turn_y(ry) * 2 + 1 - self.c

    def at(self, rx=0, rz=0, ry=0):
        return (
            lax.rem(self.x + rx, 4) * 2 + self.c,
            self.flip_z(rz) * 4 + self.turn_y(ry),
            self.g,
        )

    def twin(self):
        return (self.x * 2 + 1 - self.c, self.fs, self.g)

    def across(self, core):
        return (self.x * 2 + core, (1 - self.zl) * 4 + self.y, 1 - self.g)


class Sends:
    def __init__(self, send_sem, recv_sem):
        self.send_sem, self.recv_sem, self.count, self.open = send_sem, recv_sem, 0, []

    def make(self, src, dst, device):
        k = self.count
        self.count += 1
        return pltpu.make_async_remote_copy(
            src_ref=src,
            dst_ref=dst,
            send_sem=self.send_sem.at[k],
            recv_sem=self.recv_sem.at[k],
            device_id=device,
            device_id_type=MESH,
        )

    def start(self, src, dst, device):
        copy = self.make(src, dst, device)
        copy.start()
        self.open.append(copy)
        return copy

    def finish(self):
        for copy in self.open:
            copy.wait_send()


def greet(devices):
    barrier = pltpu.get_barrier_semaphore()
    for device in devices:
        pl.semaphore_signal(barrier, inc=1, device_id=device, device_id_type=MESH)
    pl.semaphore_wait(barrier, len(devices))


def greet_plane(me, extra=()):
    barrier = pltpu.get_barrier_semaphore()

    @pl.loop(1, 32)
    def _(k):
        q = lax.rem(me.c * 16 + me.fm + k, 32)
        fm = lax.rem(q, 16)
        device = (me.x * 2 + lax.div(q, 16), lax.div(fm, 2), lax.rem(fm, 2))
        pl.semaphore_signal(barrier, inc=1, device_id=device, device_id_type=MESH)

    for device in extra:
        pl.semaphore_signal(barrier, inc=1, device_id=device, device_id_type=MESH)
    pl.semaphore_wait(barrier, 31 + len(extra))


class BlockGather:
    def __init__(self, me, full, sends):
        self.me, self.full, self.sends, self.got, self.twins = me, full, sends, {}, []

    def send(self, key, rz, ry, start, end, device):
        part = self.full.at[self.me.slot(rz, ry), pl.ds(start, end - start)]
        self.got[key] = self.sends.start(part, part, device)

    def wait(self, *keys):
        for key in keys:
            self.got[key].wait_recv()

    def share(self, rz, ry):
        block = self.full.at[self.me.slot(rz, ry)]
        self.twins.append(self.sends.start(block, block, self.me.twin()))

    def first(self):
        me = self.me
        self.up, self.down, self.over = me.at(ry=1), me.at(ry=3), me.at(rz=1)
        self.send("ay0", 0, 0, 0, A_END, self.up)
        self.send("ay1", 0, 0, 0, A_END, self.down)
        self.send("bz", 0, 0, A_END, 128, self.over)
        self.send("az0", 0, 0, 0, A_END, self.over)
        self.send("by0", 0, 0, A_END, 128, self.up)
        self.send("by1", 0, 0, A_END, 128, self.down)
        self.share(0, 0)

    def second(self):
        self.wait("ay0")
        self.send("af0", 0, 3, 0, A_MID, self.up)
        self.send("az3", 0, 3, 0, A_END, self.over)
        self.wait("ay1")
        self.send("af1", 0, 1, A_MID, A_END, self.down)
        self.send("az1", 0, 1, 0, A_END, self.over)
        self.wait("bz")
        self.send("by2", 1, 0, A_END, 128, self.up)
        self.send("by3", 1, 0, A_END, 128, self.down)

    def third(self):
        self.wait("af0", "af1")
        self.send("az2", 0, 2, 0, A_END, self.over)
        self.wait("by0")
        self.send("bf0", 0, 3, A_END, B_MID, self.up)
        self.wait("by1")
        self.send("bf1", 0, 1, B_MID, 128, self.down)
        self.share(0, 1)
        self.share(0, 3)
        self.wait("az0")
        self.share(1, 0)

    def fourth(self):
        self.wait("by2")
        self.send("bf2", 1, 3, A_END, B_MID, self.up)
        self.wait("by3")
        self.send("bf3", 1, 1, B_MID, 128, self.down)
        self.wait("az3", "az1")
        self.share(1, 1)
        self.share(1, 3)

    def fifth(self):
        self.wait("bf0", "bf1")
        self.share(0, 2)

    def last(self):
        self.wait("az2", "bf2", "bf3")
        self.share(1, 2)
        for copy in self.twins:
            copy.wait_recv()


def gather_kernel(
    tok,
    small,
    mark,
    stored,
    first,
    second,
    xown,
    sfull,
    wlog,
    tables,
    q,
    k,
    vt,
    moments,
    xfull,
    wq,
    wk,
    wv,
    wo,
    wown,
    marks,
    holder,
    send_sem,
    recv_sem,
    local_sem,
    ex_send,
    ex_recv,
    small_send,
    small_recv,
    mark_send,
    mark_recv,
    mom_send,
    mom_recv,
):
    me = Place()
    sends = Sends(send_sem, recv_sem)
    greet_plane(
        me,
        [
            (lax.rem(me.x + rx, 4) * 2 + core, me.fs, me.g)
            for rx in (1, 2, 3)
            for core in (0, 1)
        ],
    )
    width = wlog.shape[2]
    wfull = (wq, wk, wv, wo)

    def columns(t):
        return pl.ds(pl.multiple_of(t * width, width), width)

    keep = pltpu.make_async_copy(tok, xfull.at[me.fm], local_sem.at[0])
    swap = sends.make(tok, xfull.at[me.fm], me.across(1 - me.c))

    @pl.when(me.n == 0)
    def _():
        keep.start()

    @pl.when(me.n == 1)
    def _():
        swap.start()

    place = me.dp * 16 + me.fm

    def mark_plane(j):
        t = lax.rem(me.fm + j, 16)
        return pltpu.make_async_remote_copy(
            src_ref=mark,
            dst_ref=marks.at[place],
            send_sem=mark_send.at[j],
            recv_sem=mark_recv.at[j],
            device_id=(me.dp, lax.div(t, 2), lax.rem(t, 2)),
            device_id_type=MESH,
        )

    def mark_rest(j):
        plane = marks.at[pl.ds(me.dp * 16, 16)]
        return pltpu.make_async_remote_copy(
            src_ref=plane,
            dst_ref=plane,
            send_sem=mark_send.at[16 + j],
            recv_sem=mark_recv.at[16 + j],
            device_id=(lax.rem(me.dp + j, 8), me.fs, me.g),
            device_id_type=MESH,
        )

    def exchange(j):
        t = lax.rem(me.fm + j, 16)
        return pltpu.make_async_remote_copy(
            src_ref=stored.at[:, :, columns(t)],
            dst_ref=wown.at[:, me.fm],
            send_sem=ex_send.at[j],
            recv_sem=ex_recv.at[j],
            device_id=(me.dp, lax.div(t, 2), lax.rem(t, 2)),
            device_id_type=MESH,
        )

    def move_moments(j, which):
        t = lax.rem(me.fm + j, 16)
        return pltpu.make_async_remote_copy(
            src_ref=(first, second)[which].at[:, :, columns(t)],
            dst_ref=moments.at[me.fm, pl.ds(which * 4, 4)],
            send_sem=mom_send.at[which * 16 + j],
            recv_sem=mom_recv.at[which * 16 + j],
            device_id=(me.dp, lax.div(t, 2), lax.rem(t, 2)),
            device_id_type=MESH,
        )

    mark_own = pltpu.make_async_copy(mark, marks.at[place], local_sem.at[1])
    mark_own.start()

    @pl.loop(1, 16)
    def _(j):
        mark_plane(j).start()

    @pl.loop(1, 16)
    def _(j):
        exchange(j).start()

    own = pltpu.make_async_copy(
        stored.at[:, :, columns(me.fm)], wown.at[:, me.fm], local_sem.at[2]
    )
    own.start()

    def tell(j):
        p = lax.rem(me.c * 8 + me.fs + j, 16)
        return pltpu.make_async_remote_copy(
            src_ref=small,
            dst_ref=sfull.at[me.fm],
            send_sem=small_send.at[j],
            recv_sem=small_recv.at[me.fm],
            device_id=(me.x * 2 + lax.div(p, 8), lax.rem(p, 8), me.c),
            device_id_type=MESH,
        )

    note = pltpu.make_async_copy(small, sfull.at[me.fm], local_sem.at[3])

    @pl.when(me.n == 1)
    def _():
        tell(0).start()

    @pl.when(me.n == 0)
    def _():
        note.start()

    @pl.loop(1, 16)
    def _(j):
        tell(j).start()

    @pl.when(me.n == 0)
    def _():
        keep.wait()

    @pl.when(me.n == 1)
    def _():
        swap.wait_recv()

    blocks = BlockGather(me, xfull, sends)
    blocks.first()
    hold = pltpu.make_async_copy(xfull.at[me.slot(0, 0)], xown, local_sem.at[4])
    hold.start()

    mark_own.wait()

    @pl.loop(1, 16)
    def _(j):
        mark_plane(j).wait_recv()

    @pl.loop(1, 8)
    def _(j):
        mark_rest(j).start()

    own.wait()

    @pl.loop(1, 16)
    def _(j):
        exchange(j).wait_recv()

    def far(m, core):
        return pltpu.make_async_remote_copy(
            src_ref=wown.at[m],
            dst_ref=wfull[m].at[pl.ds(me.dp * 16, 16)],
            send_sem=ex_send.at[16 + m],
            recv_sem=ex_recv.at[16 + m * 2 + core],
            device_id=me.across(me.g),
            device_id_type=MESH,
        )

    def near(m):
        return pltpu.make_async_remote_copy(
            src_ref=wown.at[m],
            dst_ref=wfull[m].at[pl.ds(me.dp * 16, 16)],
            send_sem=ex_send.at[20 + m],
            recv_sem=ex_recv.at[24 + m],
            device_id=me.twin(),
            device_id_type=MESH,
        )

    def stay(m):
        return pltpu.make_async_copy(
            wown.at[m], wfull[m].at[pl.ds(me.dp * 16, 16)], local_sem.at[6 + m]
        )

    for m in range(4):
        far(m, me.c).start()

        @pl.when(me.n == 1)
        def _():
            near(m).start()

        @pl.when(me.n == 0)
        def _():
            stay(m).start()

    right, left = me.at(rx=1), me.at(rx=3)
    ring = {}

    def both_ways(m):
        @pl.when(me.n == 1)
        def _():
            far(m, 0).wait_recv()
            far(m, 1).wait_recv()

        @pl.when(me.n == 0)
        def _():
            near(m).wait_recv()
            stay(m).wait()

        pair = wfull[m].at[pl.ds(me.x * 32, 32)]
        ring[m] = [sends.start(pair, pair, right), sends.start(pair, pair, left)]

    def pass_on(m):
        ring[m][0].wait_recv()
        one = wfull[m].at[pl.ds(lax.rem(me.x + 3, 4) * 32, 16)]
        on_right = sends.start(one, one, right)
        ring[m][1].wait_recv()
        two = wfull[m].at[pl.ds(lax.rem(me.x + 1, 4) * 32 + 16, 16)]
        on_left = sends.start(two, two, left)
        ring[m] = [on_right, on_left]

    rows = stored.shape[1]

    def in_order(m):
        for copy in ring[m]:
            copy.wait_recv()

        @pl.loop(0, 128)
        def _(b):
            wlog[m, pl.ds(pl.multiple_of(b * rows, 8), rows)] = wfull[m][holder[0, b]]

    blocks.second()
    for m in range(3):
        both_ways(m)

    @pl.loop(1, 8)
    def _(j):
        mark_rest(j).wait_recv()

    lane = lax.broadcasted_iota(jnp.int32, (8, 128), 1)
    line = lax.broadcasted_iota(jnp.int32, (8, 128), 0)
    found = lax.fori_loop(
        0,
        128,
        lambda p, total: total + jnp.where(marks[p] == lane, p, 0),
        jnp.zeros((8, 128), jnp.int32),
    )
    residues = jnp.zeros((8, 128), jnp.int32)
    for i in range(8):
        residues += jnp.where(lane == i, marks[i * 16], 0)
    tables[...] = jnp.where(line == 0, jnp.minimum(found, 127), residues)
    tell_scalar = pltpu.make_async_copy(tables, holder, local_sem.at[5])
    tell_scalar.start()

    blocks.third()
    pass_on(0)
    blocks.fourth()
    pass_on(1)
    blocks.fifth()

    @pl.loop(1, 16)
    def _(j):
        for which in (0, 1):
            move_moments(j, which).start()

    keep_moments = [
        pltpu.make_async_copy(
            source.at[:, :, columns(me.fm)],
            moments.at[me.fm, pl.ds(which * 4, 4)],
            local_sem.at[10 + which],
        )
        for which, source in enumerate((first, second))
    ]
    for copy in keep_moments:
        copy.start()

    pass_on(2)
    both_ways(3)
    blocks.last()
    tell_scalar.wait()

    def project(m, write):
        @pl.loop(0, 4)
        def _(i):
            block = xfull[pl.ds(i * 4, 4)].reshape(512, xfull.shape[2])
            value = jnp.dot(block, wlog[m], preferred_element_type=jnp.float32)
            write(pl.ds(pl.multiple_of(i * 512, 512), 512), value.astype(q.dtype))

    def write_q(part, value):
        q[part] = value

    def write_k(part, value):
        k[part] = value

    def write_v(part, value):
        vt[:, part] = value.T

    in_order(0)
    project(0, write_q)
    in_order(1)
    project(1, write_k)
    in_order(2)
    project(2, write_v)
    pass_on(3)
    in_order(3)

    @pl.loop(0, 16)
    def _(j):
        @pl.when(jnp.logical_or(me.n == 1, j != me.fm))
        def _():
            pltpu.make_async_remote_copy(
                src_ref=small,
                dst_ref=sfull.at[j],
                send_sem=small_send.at[0],
                recv_sem=small_recv.at[j],
                device_id=me.twin(),
                device_id_type=MESH,
            ).wait_recv()

    @pl.loop(1, 16)
    def _(j):
        for which in (0, 1):
            move_moments(j, which).wait_recv()

    for copy in keep_moments:
        copy.wait()

    @pl.loop(1, 16)
    def _(j):
        exchange(j).wait_send()
        tell(j).wait_send()
        mark_plane(j).wait_send()
        for which in (0, 1):
            move_moments(j, which).wait_send()

    @pl.loop(1, 8)
    def _(j):
        mark_rest(j).wait_send()

    for m in range(4):
        far(m, me.c).wait_send()

    @pl.when(me.n == 1)
    def _():
        tell(0).wait_send()
        swap.wait_send()
        for m in range(4):
            near(m).wait_send()

    @pl.when(me.n == 0)
    def _():
        note.wait()

    hold.wait()
    sends.finish()


def params(collective_id):
    return pltpu.CompilerParams(
        collective_id=collective_id, has_side_effects=True, vmem_limit_bytes=60 * 2**20
    )


def gather_inputs(tokens, small, mark, stored, first, second):
    rows, width = tokens.shape
    matrices, old_rows, columns = stored.shape
    cols = columns // 16
    dtype = tokens.dtype
    return pl.pallas_call(
        gather_kernel,
        name="gather_inputs",
        out_shape=(
            jax.ShapeDtypeStruct((rows, width), dtype),
            jax.ShapeDtypeStruct((16, *small.shape), small.dtype),
            jax.ShapeDtypeStruct((matrices, width, cols), dtype),
            jax.ShapeDtypeStruct((8, 128), jnp.int32),
            jax.ShapeDtypeStruct((16 * rows, cols), dtype),
            jax.ShapeDtypeStruct((16 * rows, cols), dtype),
            jax.ShapeDtypeStruct((cols, 16 * rows), dtype),
            jax.ShapeDtypeStruct((16, 2 * matrices, old_rows, cols), first.dtype),
        ),
        in_specs=[VMEM] * 4 + [ANY] * 2,
        out_specs=(ANY,) + (VMEM,) * 6 + (ANY,),
        scratch_shapes=[
            pltpu.VMEM((16, rows, width), dtype),
            pltpu.VMEM((128, old_rows, cols), dtype),
            pltpu.VMEM((128, old_rows, cols), dtype),
            pltpu.VMEM((128, old_rows, cols), dtype),
            pltpu.VMEM((128, old_rows, cols), dtype),
            pltpu.VMEM((matrices, 16, old_rows, cols), dtype),
            pltpu.VMEM((128, 8, 128), jnp.int32),
            pltpu.SMEM((8, 128), jnp.int32),
            pltpu.SemaphoreType.DMA((48,)),
            pltpu.SemaphoreType.DMA((48,)),
            pltpu.SemaphoreType.DMA((12,)),
            pltpu.SemaphoreType.DMA((24,)),
            pltpu.SemaphoreType.DMA((28,)),
            pltpu.SemaphoreType.DMA((16,)),
            pltpu.SemaphoreType.DMA((16,)),
            pltpu.SemaphoreType.DMA((24,)),
            pltpu.SemaphoreType.DMA((24,)),
            pltpu.SemaphoreType.DMA((32,)),
            pltpu.SemaphoreType.DMA((32,)),
        ],
        compiler_params=params(0),
    )(tokens, small, mark, stored, first, second)


def add_rows(into, start, end, *others):
    @pl.loop(0, (end - start) // 16)
    def _(i):
        rows = pl.ds(pl.multiple_of(start + i * 16, 16), 16)
        total = into[rows].astype(jnp.float32)
        for other in others:
            total += other[pl.ds(pl.multiple_of(i * 16, 16), 16)].astype(jnp.float32)
        into[rows] = total.astype(into.dtype)


def scatter_kernel(
    tables, att, w_all, hw, out, hwx, nw, w, tw, parts, r, za, zb, fa0, fa1, ya, fb0, fb1, yb, send_sem, recv_sem, local_sem, hs, hr
):
    me = Place()
    sends = Sends(send_sem, recv_sem)
    up, down, over, twin = me.at(ry=1), me.at(ry=3), me.at(rz=1), me.twin()
    right, left, partner = me.at(rx=1), me.at(rx=3), me.across(me.c)
    fetch = [
        pltpu.make_async_copy(w_all.at[part], w.at[part], local_sem.at[j])
        for j, part in enumerate((pl.ds(3, 1), pl.ds(0, 3)))
    ]
    for copy in fetch:
        copy.start()
    greet([up, down, over, twin, right, left, partner])

    order = [(1, 2), (1, 0), (1, 1), (1, 3), (0, 2), (0, 1), (0, 3), (0, 0)]
    quarter = hw.shape[0] // 4
    half = quarter // 2

    def head_copy(k, start, size, device, src):
        rows = pl.ds(start, size)
        return pltpu.make_async_remote_copy(
            src_ref=src.at[rows],
            dst_ref=hwx.at[rows],
            send_sem=hs.at[k],
            recv_sem=hr.at[k],
            device_id=device,
            device_id_type=MESH,
        )

    head_out = head_copy(0, me.x * quarter, quarter, partner, hw)
    head_right = head_copy(1, me.x * quarter, quarter, right, hwx)
    head_left = head_copy(2, me.x * quarter, quarter, left, hwx)
    head_right2 = head_copy(3, lax.rem(me.x + 3, 4) * quarter, half, right, hwx)
    head_left2 = head_copy(4, lax.rem(me.x + 1, 4) * quarter + half, half, left, hwx)

    @pl.when(me.n == 0)
    def _():
        head_out.start()

    def project(slot, write):
        @pl.loop(0, out.shape[1] // 512)
        def _(i):
            part = pl.ds(pl.multiple_of(i * 512, 512), 512)
            write(
                part,
                lax.dot_general(
                    att[slot],
                    w[3, part],
                    (((1,), (1,)), ((), ())),
                    preferred_element_type=jnp.float32,
                ),
            )

    def halve(rz, ry):
        j = rz * 4 + ry

        def write(part, value):
            parts[j, :, part] = value.astype(parts.dtype)

        project(me.other_slot(rz, ry), write)
        return sends.start(parts.at[j], r.at[j], twin)

    def merge(rz, ry):
        j = rz * 4 + ry

        def write(part, value):
            total = r[j, :, part].astype(jnp.float32) + value
            r[j, :, part] = total.astype(r.dtype)

        project(me.slot(rz, ry), write)

    a_got, b_got, y_got = {}, {}, {}
    fetch[0].wait()
    halves = [halve(*order[0]), halve(*order[1])]
    for at, (rz, ry) in enumerate(order):
        if at + 2 < 8:
            halves.append(halve(*order[at + 2]))
        halves[at].wait_recv()
        block = r.at[rz * 4 + ry]
        merge(rz, ry)
        if rz == 1:
            a_got[ry] = sends.start(block.at[pl.ds(0, A_END)], za.at[ry], over)
        if ry == 2:
            b_got[rz, 0] = sends.start(block.at[pl.ds(A_END, B_MID - A_END)], fb0.at[rz], up)
            b_got[rz, 1] = sends.start(block.at[pl.ds(B_MID, 128 - B_MID)], fb1.at[rz], down)

    @pl.when(me.n == 1)
    def _():
        head_out.wait_recv()
        head_right.start()
        head_left.start()

    give = sends.make(tw, nw, twin)
    fetch[1].wait()

    @pl.when(me.n == 0)
    def _():
        lane = lax.broadcasted_iota(jnp.int32, (64, 256), 1)
        line = lax.broadcasted_iota(jnp.int32, (64, 256), 0)
        mine, other = tables[1, me.dp], tables[1, me.x * 2 + 1 - me.c]
        wanted = jnp.where(line < 32, line * 8 + mine, (line - 32) * 8 + other)
        pick = jnp.where(lane == wanted, 1.0, 0.0).astype(w.dtype)
        for m in range(4):

            @pl.loop(0, w.shape[1] // 256)
            def _(t):
                rows = pl.ds(pl.multiple_of(t * 256, 256), 256)
                chosen = jnp.dot(pick, w[m, rows], preferred_element_type=jnp.float32)
                chosen = chosen.astype(nw.dtype)
                to = pl.ds(pl.multiple_of(t * 32, 32), 32)
                nw[m, to] = chosen[:32]
                tw[m, to] = chosen[32:]

        give.start()

    tail = pl.ds(A_END, 128 - A_END)
    for rz in (1, 0):
        b_got[rz, 0].wait_recv()
        add_rows(r.at[rz * 4 + 1], A_END, B_MID, fb0.at[rz])
        y_got[rz, 0] = sends.start(r.at[rz * 4 + 1, tail], yb.at[rz * 2], up)
        b_got[rz, 1].wait_recv()
        add_rows(r.at[rz * 4 + 3], B_MID, 128, fb1.at[rz])
        y_got[rz, 1] = sends.start(r.at[rz * 4 + 3, tail], yb.at[rz * 2 + 1], down)

    head = pl.ds(0, A_END)
    a_got[2].wait_recv()
    add_rows(r.at[2], 0, A_END, za.at[2])
    f_up = sends.start(r.at[2, pl.ds(0, A_MID)], fa0, up)
    f_down = sends.start(r.at[2, pl.ds(A_MID, A_END - A_MID)], fa1, down)

    y_got[1, 0].wait_recv()
    y_got[1, 1].wait_recv()
    add_rows(r.at[4], A_END, 128, yb.at[2], yb.at[3])
    z_got = sends.start(r.at[4, tail], zb, over)

    @pl.when(me.n == 1)
    def _():
        head_right.wait_recv()
        head_right2.start()
        head_left.wait_recv()
        head_left2.start()

    a_got[1].wait_recv()
    add_rows(r.at[1], 0, A_END, za.at[1])
    f_up.wait_recv()
    add_rows(r.at[1], 0, A_MID, fa0)
    g_up = sends.start(r.at[1, head], ya.at[0], up)
    a_got[3].wait_recv()
    add_rows(r.at[3], 0, A_END, za.at[3])
    f_down.wait_recv()
    add_rows(r.at[3], A_MID, A_END, fa1)
    g_down = sends.start(r.at[3, head], ya.at[1], down)

    def total(start, end, others):
        @pl.loop(0, (end - start) // 16)
        def _(i):
            here = pl.ds(pl.multiple_of(i * 16, 16), 16)
            rows = pl.ds(pl.multiple_of(start + i * 16, 16), 16)
            value = r[0, rows].astype(jnp.float32)
            for other in others:
                value += other[here].astype(jnp.float32)
            out[rows] = value

    y_got[0, 0].wait_recv()
    y_got[0, 1].wait_recv()
    z_got.wait_recv()
    total(A_END, 128, [yb.at[0], yb.at[1], zb])
    a_got[0].wait_recv()
    g_up.wait_recv()
    g_down.wait_recv()
    total(0, A_END, [za.at[0], ya.at[0], ya.at[1]])

    @pl.when(me.n == 1)
    def _():
        give.wait_recv()
        head_right2.wait_recv()
        head_left2.wait_recv()
        head_right.wait_send()
        head_left.wait_send()
        head_right2.wait_send()
        head_left2.wait_send()

    @pl.when(me.n == 0)
    def _():
        give.wait_send()
        head_out.wait_send()

    sends.finish()


def scatter_parts(tables, att, w, hw):
    rows, width = att.shape[1], w.shape[1]
    kept = (w.shape[0], width // 8, w.shape[2])
    dtype = att.dtype
    return pl.pallas_call(
        scatter_kernel,
        name="scatter_parts",
        out_shape=(
            jax.ShapeDtypeStruct((rows, width), jnp.float32),
            jax.ShapeDtypeStruct(hw.shape, hw.dtype),
            jax.ShapeDtypeStruct(kept, w.dtype),
        ),
        in_specs=[SMEM, VMEM, ANY, ANY],
        out_specs=(VMEM, ANY, VMEM),
        scratch_shapes=[
            pltpu.VMEM(w.shape, w.dtype),
            pltpu.VMEM(kept, w.dtype),
            pltpu.VMEM((8, rows, width), dtype),
            pltpu.VMEM((8, rows, width), dtype),
            pltpu.VMEM((4, A_END, width), dtype),
            pltpu.VMEM((rows - A_END, width), dtype),
            pltpu.VMEM((A_MID, width), dtype),
            pltpu.VMEM((A_END - A_MID, width), dtype),
            pltpu.VMEM((2, A_END, width), dtype),
            pltpu.VMEM((2, B_MID - A_END, width), dtype),
            pltpu.VMEM((2, rows - B_MID, width), dtype),
            pltpu.VMEM((4, rows - A_END, width), dtype),
            pltpu.SemaphoreType.DMA((32,)),
            pltpu.SemaphoreType.DMA((32,)),
            pltpu.SemaphoreType.DMA((2,)),
            pltpu.SemaphoreType.DMA((5,)),
            pltpu.SemaphoreType.DMA((5,)),
        ],
        compiler_params=params(2),
    )(tables, att, w, hw)


def finish_kernel(
    tables,
    summed,
    xown,
    gain,
    tcol,
    hw_own,
    hw_far,
    moments_all,
    loss,
    new_first,
    new_second,
    hw,
    moments,
    packed,
    got_moments,
    full,
    lg,
    cols,
    st,
    got,
    send_sem,
    recv_sem,
    local_sem,
    tell_send,
    tell_recv,
):
    me = Place()
    sends = Sends(send_sem, recv_sem)

    def fetch_head(source):
        return pltpu.make_async_copy(source, hw, local_sem.at[1])

    @pl.when(me.n == 0)
    def _():
        fetch_head(hw_own).start()

    @pl.when(me.n == 1)
    def _():
        fetch_head(hw_far).start()

    fetch_moments = pltpu.make_async_copy(moments_all, moments, local_sem.at[2])
    fetch_moments.start()
    greet_plane(
        me,
        [
            (lax.rem(me.x + rx, 4) * 2 + core, me.fs, me.g)
            for rx in (1, 2, 3)
            for core in (0, 1)
        ],
    )
    own = me.slot(0, 0)
    width = summed.shape[1]

    @pl.loop(0, 8)
    def _(i):
        rows = pl.ds(pl.multiple_of(i * 16, 16), 16)
        hidden = xown[rows].astype(jnp.float32) + summed[rows]
        mean = jnp.sum(hidden * hidden, axis=1, keepdims=True) * (1.0 / width)
        normed = hidden * lax.rsqrt(mean + 1e-05) * gain[...]
        full[own, rows] = normed.astype(full.dtype)

    blocks = BlockGather(me, full, sends)
    vocab = hw.shape[1]
    sender = me.c * 8 + me.fs

    def tell(b):
        return pltpu.make_async_remote_copy(
            src_ref=st.at[b],
            dst_ref=got.at[sender],
            send_sem=tell_send.at[b],
            recv_sem=tell_recv.at[sender],
            device_id=(me.x * 2 + me.g, lax.div(b, 2), lax.rem(b, 2)),
            device_id_type=MESH,
        )

    note = pltpu.make_async_copy(st.at[me.fm], got.at[sender], local_sem.at[0])

    def score(*pairs):
        slots = [slot(rz, ry) for rz, ry in pairs for slot in (me.slot, me.other_slot)]
        rows = pl.ds(0, 128 * len(slots))

        @pl.loop(0, vocab // 256)
        def _(i):
            part = pl.ds(pl.multiple_of(i * 256, 256), 256)
            block = jnp.concatenate([full[slot] for slot in slots], axis=0)
            lg[rows, part] = jnp.dot(block, hw[:, part], preferred_element_type=jnp.float32)

        for t, slot in enumerate(slots):

            @pl.loop(0, 4)
            def _(i):
                here = pl.ds(pl.multiple_of(t * 128 + i * 32, 32), 32)
                to = pl.ds(pl.multiple_of(i * 32, 32), 32)
                parts = [lg[here, pl.ds(j * 128, 128)] for j in range(vocab // 128)]
                top = parts[0]
                for part in parts[1:]:
                    top = jnp.maximum(top, part)
                wanted = tcol[slot, to] - own * vocab
                ids = lax.broadcasted_iota(jnp.int32, top.shape, 1)
                total, picked = jnp.zeros_like(top), jnp.zeros_like(top)
                for j, part in enumerate(parts):
                    total += jnp.exp(part - top)
                    picked += jnp.where(ids + j * 128 == wanted, part, 0.0)
                cols[0, to], cols[1, to], cols[2, to] = top, total, picked

            tops = cols[0].T
            top = jnp.max(tops, axis=0, keepdims=True)
            total = jnp.sum(cols[1].T * jnp.exp(tops - top), axis=0, keepdims=True)
            picked = jnp.sum(cols[2].T, axis=0, keepdims=True)
            st[slot] = jnp.concatenate([top, total, picked, jnp.zeros((5, 128))], axis=0)

            @pl.when(jnp.logical_or(me.n == 1, slot != me.fm))
            def _():
                tell(slot).start()

            @pl.when(jnp.logical_and(me.n == 0, slot == me.fm))
            def _():
                note.start()

    def twins(*which):
        for k in which:
            blocks.twins[k].wait_recv()

    mine = pl.ds(me.dp * 16, 16)

    def to_dp(j):
        dp = lax.rem(me.dp + j, 8)
        return pltpu.make_async_remote_copy(
            src_ref=packed.at[dp],
            dst_ref=got_moments.at[mine],
            send_sem=send_sem.at[32 + j],
            recv_sem=recv_sem.at[32 + j],
            device_id=(dp, me.fs, me.g),
            device_id_type=MESH,
        )

    keep_moments = pltpu.make_async_copy(
        packed.at[me.dp], got_moments.at[mine], local_sem.at[3]
    )

    blocks.first()

    fetch_moments.wait()

    @pl.loop(0, 16)
    def _(p):
        for i in range(8):
            residue = tables[1, i]
            for m in range(8):
                for j in range(3):
                    packed[i, p, pl.ds(m * 3 + j, 1)] = moments[p, m, pl.ds(j * 8 + residue, 1)]

    @pl.loop(1, 8)
    def _(j):
        to_dp(j).start()

    keep_moments.start()
    fetch_head(hw_own).wait()
    twins(0)
    score((0, 0))
    blocks.second()
    blocks.third()
    twins(1, 2)
    score((0, 1), (0, 3))
    blocks.fourth()
    blocks.fifth()
    twins(3, 4)
    score((1, 0), (1, 1))
    blocks.wait("az2", "bf2", "bf3")
    blocks.share(1, 2)

    keep_moments.wait()

    @pl.loop(1, 8)
    def _(j):
        to_dp(j).wait_recv()

    @pl.loop(0, 16)
    def _(t):
        holders = [tables[0, t * 8 + u] for u in range(8)]
        rows = pl.ds(pl.multiple_of(t * 24, 8), 24)
        for s, target in enumerate((new_first, new_second)):
            for m in range(4):
                target[m, rows] = jnp.concatenate(
                    [got_moments[p, pl.ds(s * 12 + m * 3, 3)] for p in holders], axis=0
                )

    twins(5, 6)
    score((1, 3), (0, 2))
    twins(7)
    score((1, 2))

    @pl.loop(0, 16)
    def _(j):
        @pl.when(jnp.logical_or(me.n == 1, j != sender))
        def _():
            pltpu.make_async_remote_copy(
                src_ref=st.at[0],
                dst_ref=got.at[j],
                send_sem=tell_send.at[0],
                recv_sem=tell_recv.at[j],
                device_id=me.twin(),
                device_id_type=MESH,
            ).wait_recv()

    @pl.when(me.n == 0)
    def _():
        note.wait()

    top = got[0, 0:1]
    for j in range(1, 16):
        top = jnp.maximum(top, got[j, 0:1])
    total, picked = jnp.zeros_like(top), jnp.zeros_like(top)
    for j in range(16):
        total += got[j, 1:2] * jnp.exp(got[j, 0:1] - top)
        picked += got[j, 2:3]
    loss[...] = jnp.broadcast_to(top + jnp.log(total) - picked, loss.shape)

    @pl.loop(0, 16)
    def _(b):
        @pl.when(jnp.logical_or(me.n == 1, b != me.fm))
        def _():
            tell(b).wait_send()

    @pl.loop(1, 8)
    def _(j):
        to_dp(j).wait_send()

    sends.finish()


def finish(tables, summed, xown, gain, tcol, hw_own, hw_far, moments):
    rows, width = summed.shape
    holders, sets, old_rows, cols = moments.shape
    dtype = moments.dtype
    kept = jax.ShapeDtypeStruct((sets // 2, width // 8, cols), dtype)
    return pl.pallas_call(
        finish_kernel,
        name="finish",
        out_shape=(jax.ShapeDtypeStruct((8, rows), jnp.float32), kept, kept),
        in_specs=[SMEM] + [VMEM] * 4 + [ANY] * 3,
        out_specs=(VMEM,) * 3,
        scratch_shapes=[
            pltpu.VMEM(hw_own.shape, hw_own.dtype),
            pltpu.VMEM(moments.shape, dtype),
            pltpu.VMEM((8, holders, sets * 3, cols), dtype),
            pltpu.VMEM((8 * holders, sets * 3, cols), dtype),
            pltpu.VMEM((16, rows, width), jnp.bfloat16),
            pltpu.VMEM((4 * rows, hw_own.shape[1]), jnp.float32),
            pltpu.VMEM((3, rows, 128), jnp.float32),
            pltpu.VMEM((16, 8, rows), jnp.float32),
            pltpu.VMEM((16, 8, rows), jnp.float32),
            pltpu.SemaphoreType.DMA((40,)),
            pltpu.SemaphoreType.DMA((40,)),
            pltpu.SemaphoreType.DMA((4,)),
            pltpu.SemaphoreType.DMA((16,)),
            pltpu.SemaphoreType.DMA((16,)),
        ],
        compiler_params=params(1),
    )(tables, summed, xown, gain, tcol, hw_own, hw_far, moments)


def attend_kernel(begin, q, k, vt, seg_row, seg_col, out):
    heads = out.shape[1] // HD
    seq = q.shape[0]
    size = 256
    scale = math.log2(math.e) / math.sqrt(HD)
    ahead = lax.broadcasted_iota(jnp.int32, (size, size), 0) - lax.broadcasted_iota(
        jnp.int32, (size, size), 1
    )

    @pl.loop(0, seq // size)
    def _(i):
        rows = pl.ds(pl.multiple_of(i * size, size), size)
        own = seg_row[0:1, rows]

        def step(j, carry):
            cols = pl.ds(pl.multiple_of(j * size, size), size)
            allowed = (ahead <= (i - j) * size) & (seg_col[cols] == own)
            result = []
            for h in range(heads):
                part = pl.ds(h * HD, HD)
                top, total, acc = carry[h]
                score = lax.dot_general(
                    k[cols, part],
                    q[rows, part],
                    (((1,), (1,)), ((), ())),
                    preferred_element_type=jnp.float32,
                )
                score = jnp.where(allowed, score * scale, -1e30)
                new_top = jnp.maximum(top, jnp.max(score, axis=0, keepdims=True))
                prob = jnp.exp2(score - new_top)
                keep = jnp.exp2(top - new_top)
                total = total * keep + jnp.sum(prob, axis=0, keepdims=True)
                acc = acc * keep + jnp.dot(
                    vt[part, cols], prob.astype(vt.dtype), preferred_element_type=jnp.float32
                )
                result.append((new_top, total, acc))
            return tuple(result)

        start = (
            jnp.full((1, size), -1e30, jnp.float32),
            jnp.zeros((1, size), jnp.float32),
            jnp.zeros((HD, size), jnp.float32),
        )
        done = lax.fori_loop(begin[i], i + 1, step, (start,) * heads)
        for h in range(heads):
            _, total, acc = done[h]
            out[rows, pl.ds(h * HD, HD)] = (acc / total).T.astype(out.dtype)


def attend(q, k, vt, segments):
    seq = q.shape[0]
    heads_of = segments.reshape(-1, 256)[:, :1]
    begin = jnp.sum((segments[None, :] < heads_of).astype(jnp.int32), axis=1) // 256
    return pl.pallas_call(
        attend_kernel,
        name="attend",
        out_shape=jax.ShapeDtypeStruct(q.shape, q.dtype),
        in_specs=[SMEM] + [VMEM] * 5,
        out_specs=VMEM,
        compiler_params=pltpu.CompilerParams(vmem_limit_bytes=60 * 2**20),
    )(begin, q, k, vt, segments[None, :], segments[:, None])


def body(
    tokens_in,
    segment_ids,
    target_ids,
    old_weights,
    old_first,
    old_second,
    old_block,
    new_residue,
    norm_gain,
    head_weight,
):
    small = jnp.stack([segment_ids, target_ids] + [segment_ids] * 6)
    mark = jnp.where(jnp.arange(8)[:, None] == 0, old_block[0], new_residue[0])
    mark = jnp.broadcast_to(mark, (8, 128)).astype(jnp.int32)
    xown, sfull, weights, tables, q, k, vt, moments = gather_inputs(
        tokens_in, small, mark, old_weights, old_first, old_second
    )
    segments = sfull[:, 0].reshape(-1)
    targets = sfull[:, 1][:, :, None]
    attended = attend(q, k, vt, segments)
    summed, head_far, new_weights = scatter_parts(
        tables, attended.reshape(16, -1, attended.shape[1]), weights, head_weight
    )
    loss, new_first, new_second = finish(
        tables, summed, xown, norm_gain[None, :], targets, head_weight, head_far, moments
    )
    return (new_weights, new_first, new_second, loss[0])


def solution(mesh):
    placed = (
        P(("dp", "fsdp", "mp"), None),
        P(("dp", "fsdp", "mp")),
        P(("dp", "fsdp", "mp")),
        P(None, ("dp", "fsdp", "mp"), None),
        P(None, ("dp", "fsdp", "mp"), None),
        P(None, ("dp", "fsdp", "mp"), None),
        P(("dp", "fsdp", "mp")),
        P("dp"),
        P(),
        P(None, ("fsdp", "mp")),
    )
    return jax.shard_map(
        body,
        mesh=mesh,
        in_specs=placed,
        out_specs=(
            P(None, "dp", ("fsdp", "mp")),
            P(None, "dp", ("fsdp", "mp")),
            P(None, "dp", ("fsdp", "mp")),
            P(("dp", "fsdp", "mp")),
        ),
        check_vma=False,
    )
```
